16 devices in a mesh: tube: 2 (over z), col: 2 (over y), row: 4 (over x, core).
Axes of the slice: x: 2, y: 2, z: 2, core: 2. Of those that a mesh axis runs over, the one named last changes fastest.
Arguments:
- tensor: float32 [32, 1024, 2048], P('tube', 'row', 'col')
- b_init: float32 [2048, 128], P(('col', 'row', 'tube'))
- c_init: float32 [32, 128], replicated
- ridge_lam: float32 [], replicated
Outputs:
- output 1: float32 [1024, 128], P(('row', 'col', 'tube'))
- output 2: float32 [2048, 128], P(('col', 'row', 'tube'))
- output 3: float32 [32, 128], replicated
All inputs are finite; a program needn't handle non-finite values.
Results may differ from the reference program's by a relative error of at most 0.001.
Values are sent between devices in bfloat16 or wider.
A program may use at most 1 GiB of HBM per device.

```python
import jax
import jax.numpy as jnp
from jax import lax

K_LEN = 32
CP_RANK = 128
I_ROWS = 1024
J_ROWS = 2048
SWEEPS = 2


def setup_inputs(seed: int = 0) -> dict:
    keys = jax.random.split(jax.random.key(seed), 7)
    scale = CP_RANK ** (-1.0 / 6.0)
    fac_a = scale * jax.random.normal(keys[0], (I_ROWS, CP_RANK), jnp.float32)
    fac_b = scale * jax.random.normal(keys[1], (J_ROWS, CP_RANK), jnp.float32)
    fac_c = scale * jax.random.normal(keys[2], (K_LEN, CP_RANK), jnp.float32)
    kir_prod = fac_c[:, None, :] * fac_a[None, :, :]
    planted = jnp.einsum("kir,jr->kij", kir_prod, fac_b)
    noise = 0.3 * jax.random.normal(keys[3], (K_LEN, I_ROWS, J_ROWS), jnp.float32)
    b_init = fac_b + scale * jax.random.normal(keys[4], (J_ROWS, CP_RANK), jnp.float32)
    c_init = fac_c + scale * jax.random.normal(keys[5], (K_LEN, CP_RANK), jnp.float32)
    ridge_lam = jax.random.uniform(keys[6], (), jnp.float32, 0.1, 0.3) * (J_ROWS * K_LEN * CP_RANK ** (-2.0 / 3.0))
    return {"tensor": planted + noise, "b_init": b_init, "c_init": c_init, "ridge_lam": ridge_lam}


def gram_of(factor):
    half_fac = factor.astype(jnp.bfloat16)
    return jnp.dot(half_fac.T, half_fac, preferred_element_type=jnp.float32)


def solve_rows(mttkrp_rows, gram_prod, ridge_lam):
    ident_mat = jnp.eye(gram_prod.shape[0], dtype=gram_prod.dtype)
    chol_fac = jnp.linalg.cholesky(gram_prod + ridge_lam * ident_mat)
    half_solve = lax.linalg.triangular_solve(chol_fac, mttkrp_rows, left_side=False, lower=True, transpose_a=True)
    return lax.linalg.triangular_solve(chol_fac, half_solve, left_side=False, lower=True)


def reference(tensor, b_init, c_init, ridge_lam):
    x_half = tensor.astype(jnp.bfloat16)
    flat_x = x_half.reshape(K_LEN * I_ROWS, J_ROWS)
    fac_b = b_init
    fac_c = c_init
    gram_b = gram_of(fac_b)
    for sweep_idx in range(SWEEPS):
        gram_c = gram_of(fac_c)
        u_kir = jnp.dot(flat_x, fac_b.astype(jnp.bfloat16), preferred_element_type=jnp.float32).reshape(K_LEN, I_ROWS, CP_RANK)
        mtt_a = jnp.einsum("kir,kr->ir", u_kir.astype(jnp.float32), fac_c.astype(jnp.float32))
        fac_a = solve_rows(mtt_a, gram_b * gram_c, ridge_lam)
        gram_a = gram_of(fac_a)
        a_half = fac_a.astype(jnp.bfloat16)
        v_kjr = lax.map(lambda slab: lax.dot_general(slab, a_half, (((0,), (0,)), ((), ())), preferred_element_type=jnp.float32), x_half)
        mtt_b = jnp.einsum("kjr,kr->jr", v_kjr.astype(jnp.float32), fac_c.astype(jnp.float32))
        fac_b = solve_rows(mtt_b, gram_a * gram_c, ridge_lam)
        gram_b = gram_of(fac_b)
        u_kir = jnp.dot(flat_x, fac_b.astype(jnp.bfloat16), preferred_element_type=jnp.float32).reshape(K_LEN, I_ROWS, CP_RANK)
        mtt_c = jnp.einsum("kir,ir->kr", u_kir.astype(jnp.float32), fac_a.astype(jnp.float32))
        fac_c = solve_rows(mtt_c, gram_a * gram_b, ridge_lam)
    return fac_a, fac_b, fac_c
```

```python
import jax
import jax.numpy as jnp
from jax import lax
from jax.experimental import pallas as pl
from jax.experimental.pallas import tpu as pltpu
from jax.sharding import PartitionSpec as P

SWEEPS = 2
HI = lax.Precision.HIGHEST
MESH = pl.DeviceIdType.MESH
F32 = jnp.float32
BF16 = jnp.bfloat16

OFF_YZ = [(t, c, 0) for c in range(2) for t in range(2)][1:]
OFF_XZ = [(t, 0, w) for w in range(4) for t in range(2)][1:]
OFF_ALL_REST = [(t, c, w) for w in range(1, 4) for c in range(2) for t in range(2)]
OFF_ALL = OFF_YZ + OFF_ALL_REST


def dot_t0(a, b, **kw):
    return lax.dot_general(a, b, (((0,), (0,)), ((), ())), preferred_element_type=F32, **kw)


def kernel(
    x_hbm, b_ref, c_ref, lam_ref,
    a_out, b_out, c_out,
    xf, xh, u_ref, bcols, a16, at_ref, af, pa, rsa, vt, rsb, gbp, gbr, pc, cb,
    w_ref, q_ref, li_ref, inv_ref, ga_ref, gb_ref, cfac,
    x_sem, rsa_s, rsa_r, aga_s, aga_r, af_s, af_r, rsb_s, rsb_r, agb_s, agb_r, gb_s, gb_r, pc_s, pc_r,
):
    t = lax.axis_index("tube")
    c = lax.axis_index("col")
    w = lax.axis_index("row")
    kk, ii, jj = xf.shape
    rank = b_ref.shape[1]
    g = c * 2 + t
    q = w * 2 + t
    me = g * 4 + w

    for k in range(kk):
        pltpu.make_async_copy(x_hbm.at[k], xf.at[k], x_sem.at[k]).start()

    def dev(off):
        return ((t + off[0]) % 2, (c + off[1]) % 2, (w + off[2]) % 4)

    barrier = pltpu.get_barrier_semaphore()
    for off in OFF_ALL:
        pl.semaphore_signal(barrier, inc=1, device_id=dev(off), device_id_type=MESH)
    pl.semaphore_wait(barrier, len(OFF_ALL))

    def push(src, dst, ss, rs, off):
        return pltpu.make_async_remote_copy(
            src_ref=src, dst_ref=dst, send_sem=ss, recv_sem=rs, device_id=dev(off), device_id_type=MESH
        )

    def gather_b(s):
        return [
            push(bcols.at[s, q], bcols.at[s, q], agb_s.at[s, n], agb_r.at[s, n], off)
            for n, off in enumerate(OFF_XZ)
        ]

    def gram_copy(s):
        return push(gbp, gbr.at[s], gb_s.at[s], gb_r.at[s], (0, 1, 0))

    def u_pass(s):
        bmat = bcols[s].reshape(jj, rank)

        def body(k, _):
            u_ref[k] = jnp.dot(xh[k], bmat, preferred_element_type=F32)
            return 0

        lax.fori_loop(0, kk, body, 0)

    def start_gram_b(s):
        bmat = bcols[s].reshape(jj, rank)
        gbp[...] = dot_t0(bmat, bmat)
        gram_copy(s).start()

    def finish_gram_b(s):
        gram_copy(s).wait()
        gb_ref[...] = gbp[...] + gbr[s]

    def factor(gram_prod):
        rows = lax.broadcasted_iota(jnp.int32, (rank, rank), 0)
        cols = lax.broadcasted_iota(jnp.int32, (rank, rank), 1)
        eye = jnp.where(rows == cols, 1.0, 0.0).astype(F32)
        w_ref[:, :rank] = gram_prod + lam_ref[0, 0] * eye
        w_ref[:, rank:] = eye
        q_ref[...] = jnp.zeros_like(q_ref)
        r1 = lax.broadcasted_iota(jnp.int32, (8, rank), 0)
        r2 = lax.broadcasted_iota(jnp.int32, (8, 2 * rank), 0)

        def body(b, _):
            off = pl.multiple_of(b * 8, 8)
            pan = w_ref[pl.ds(off, 8), :]
            rolled = pltpu.roll(pan[:, :rank], rank - off, axis=1)
            e = [jnp.broadcast_to(rolled[:, n : n + 1], (8, rank)) for n in range(8)]
            chol = jnp.zeros_like(pan)
            for j in range(8):
                piv = jnp.broadcast_to(e[j][j : j + 1], (8, rank))
                isq = lax.rsqrt(piv)
                rc = isq * isq
                m = e[j] * rc
                m2 = jnp.concatenate([m, m], axis=1)
                isq2 = jnp.concatenate([isq, isq], axis=1)
                rc2 = jnp.concatenate([rc, rc], axis=1)
                pj = jnp.broadcast_to(pan[j : j + 1], (8, 2 * rank))
                chol = jnp.where(r2 == j, pj * isq2, chol)
                pan = jnp.where(r2 == j, pj * rc2, pan - m2 * pj)
                for n in range(j + 1, 8):
                    en = jnp.broadcast_to(e[n][j : j + 1], (8, rank))
                    e[n] = jnp.where(r1 == j, en * rc, e[n] - m * en)
            li_ref[pl.ds(off, 8), :] = chol[:, rank:]
            q_ref[pl.ds(off, 8), :] = pan
            w_ref[...] = w_ref[...] - jnp.dot(w_ref[:, :rank], q_ref[...], precision=HI, preferred_element_type=F32)
            q_ref[pl.ds(off, 8), :] = jnp.zeros_like(pan)
            return 0

        lax.fori_loop(0, rank // 8, body, 0)
        inv_ref[...] = dot_t0(li_ref[...], li_ref[...], precision=HI)

    bcols[0, q] = b_ref[...].astype(BF16)
    cps = gather_b(0)
    for cp in cps:
        cp.start()
    cfac[...] = c_ref[...]

    def load(k, _):
        pltpu.make_async_copy(x_hbm.at[k], xf.at[k], x_sem.at[k]).wait()
        xh[k] = xf[k].astype(BF16)
        return 0

    lax.fori_loop(0, kk, load, 0)
    for cp in cps:
        cp.wait()
    start_gram_b(0)
    u_pass(0)
    finish_gram_b(0)

    def sweep(s, _):
        c16 = cfac[...].astype(BF16)
        gram_c = dot_t0(c16, c16)

        def body_a(k, acc):
            return acc + u_ref[k] * cfac[pl.ds(t * kk + k, 1), :]

        part = lax.fori_loop(0, kk, body_a, jnp.zeros((ii, rank), F32))
        pa[...] = part.reshape(pa.shape)
        ra = []
        for n, off in enumerate(OFF_YZ):
            g2 = dev(off)[1] * 2 + dev(off)[0]
            ra.append(push(pa.at[g2], rsa.at[s, n], rsa_s.at[s, n], rsa_r.at[s, n], off))
        for cp in ra:
            cp.start()
        factor(gb_ref[...] * gram_c)
        for cp in ra:
            cp.wait()
        mtt_a = pa[g] + rsa[s, 0] + rsa[s, 1] + rsa[s, 2]
        a_own = jnp.dot(mtt_a, inv_ref[...], precision=HI, preferred_element_type=F32)
        a_out[...] = a_own
        a16[s, w, g] = a_own.astype(BF16)
        af[s, g] = a_own
        ga = [push(a16.at[s, w, g], a16.at[s, w, g], aga_s.at[s, n], aga_r.at[s, n], off) for n, off in enumerate(OFF_ALL)]
        for cp in ga:
            cp.start()
        fa = [push(af.at[s, g], af.at[s, g], af_s.at[s, n], af_r.at[s, n], off) for n, off in enumerate(OFF_YZ)]
        for cp in fa:
            cp.start()

        cmine = cfac[pl.ds(pl.multiple_of(t * kk, kk), kk), :]
        ct = jnp.transpose(jnp.concatenate([cmine, jnp.zeros((rank - kk, rank), F32)], axis=0))
        for k in range(kk):
            cb[k] = jnp.broadcast_to(ct[:, k : k + 1], (rank, rank))
        for cp in ga[:3]:
            cp.wait()
        at_ref[...] = jnp.transpose(a16[s, w].reshape(ii, rank))
        vt[...] = jnp.zeros_like(vt)

        def body_b(k, _):
            v = jnp.dot(at_ref[...], xh[k], preferred_element_type=F32)
            ck = cb[k]
            for n in range(jj // rank):
                vt[n] += v[:, n * rank : (n + 1) * rank] * ck
            return 0

        lax.fori_loop(0, kk, body_b, 0)
        rb = []
        for n, off in enumerate(OFF_XZ):
            q2 = dev(off)[2] * 2 + dev(off)[0]
            rb.append(push(vt.at[q2], rsb.at[s, n], rsb_s.at[s, n], rsb_r.at[s, n], off))
        for cp in rb:
            cp.start()
        for cp in ga[3:]:
            cp.wait()
        aall = a16[s].reshape(4 * ii, rank)
        ga_ref[...] = dot_t0(aall, aall)
        factor(ga_ref[...] * gram_c)
        for cp in rb:
            cp.wait()
        mtt_b = vt[q]
        for n in range(len(OFF_XZ)):
            mtt_b = mtt_b + rsb[s, n]
        b_own = jnp.transpose(jnp.dot(inv_ref[...], mtt_b, precision=HI, preferred_element_type=F32))
        b_out[...] = b_own
        bcols[s + 1, q] = b_own.astype(BF16)
        gcs = gather_b(s + 1)
        for cp in gcs:
            cp.start()
        for cp in gcs:
            cp.wait()

        start_gram_b(s + 1)
        u_pass(s + 1)
        for cp in fa:
            cp.wait()
        afull = af[s].reshape(ii, rank)
        pc[s, me] = jnp.concatenate(
            [jnp.sum(u_ref[k] * afull, axis=0, keepdims=True) for k in range(kk)], axis=0
        )
        cs = [push(pc.at[s, me], pc.at[s, me], pc_s.at[s, n], pc_r.at[s, n], off) for n, off in enumerate(OFF_ALL)]
        for cp in cs:
            cp.start()
        finish_gram_b(s + 1)
        factor(ga_ref[...] * gb_ref[...])
        for cp in cs:
            cp.wait()
        halves = []
        for t2 in range(2):
            tot = None
            for c2 in range(2):
                for w2 in range(4):
                    term = pc[s, (c2 * 2 + t2) * 4 + w2]
                    tot = term if tot is None else tot + term
            halves.append(tot)
        cfac[...] = jnp.dot(jnp.concatenate(halves, axis=0), inv_ref[...], precision=HI, preferred_element_type=F32)
        return 0

    lax.fori_loop(0, SWEEPS, sweep, 0)
    c_out[...] = cfac[...]


def solution(mesh):
    def local_sweeps(x_blk, b_own, c_full, ridge_lam):
        kk, ii, jj = x_blk.shape
        rank = b_own.shape[1]
        arows, brows = ii // 4, b_own.shape[0]
        dma = pltpu.SemaphoreType.DMA
        vmem = pl.BlockSpec(memory_space=pltpu.VMEM)
        return pl.pallas_call(
            kernel,
            name="als",
            out_shape=(
                jax.ShapeDtypeStruct((arows, rank), F32),
                jax.ShapeDtypeStruct((brows, rank), F32),
                jax.ShapeDtypeStruct(c_full.shape, F32),
            ),
            in_specs=[
                pl.BlockSpec(memory_space=pl.ANY), vmem, vmem, pl.BlockSpec(memory_space=pltpu.SMEM),
            ],
            out_specs=(vmem, vmem, vmem),
            scratch_shapes=[
                pltpu.VMEM((kk, ii, jj), F32),
                pltpu.VMEM((kk, ii, jj), BF16),
                pltpu.VMEM((kk, ii, rank), F32),
                pltpu.VMEM((SWEEPS + 1, 8, brows, rank), BF16),
                pltpu.VMEM((SWEEPS, 4, 4, arows, rank), BF16),
                pltpu.VMEM((rank, ii), BF16),
                pltpu.VMEM((SWEEPS, 4, arows, rank), F32),
                pltpu.VMEM((4, arows, rank), F32),
                pltpu.VMEM((SWEEPS, 3, arows, rank), F32),
                pltpu.VMEM((8, rank, brows), F32),
                pltpu.VMEM((SWEEPS, 7, rank, brows), F32),
                pltpu.VMEM((rank, rank), F32),
                pltpu.VMEM((SWEEPS + 1, rank, rank), F32),
                pltpu.VMEM((SWEEPS, 16, kk, rank), F32),
                pltpu.VMEM((kk, rank, rank), F32),
                pltpu.VMEM((rank, 2 * rank), F32),
                pltpu.VMEM((rank, 2 * rank), F32),
                pltpu.VMEM((rank, rank), F32),
                pltpu.VMEM((rank, rank), F32),
                pltpu.VMEM((rank, rank), F32),
                pltpu.VMEM((rank, rank), F32),
                pltpu.VMEM(c_full.shape, F32),
                dma((kk,)),
                dma((SWEEPS, 3)), dma((SWEEPS, 3)),
                dma((SWEEPS, 15)), dma((SWEEPS, 15)),
                dma((SWEEPS, 3)), dma((SWEEPS, 3)),
                dma((SWEEPS, 7)), dma((SWEEPS, 7)),
                dma((SWEEPS + 1, 7)), dma((SWEEPS + 1, 7)),
                dma((SWEEPS + 1,)), dma((SWEEPS + 1,)),
                dma((SWEEPS, 15)), dma((SWEEPS, 15)),
            ],
            compiler_params=pltpu.CompilerParams(
                collective_id=0, has_side_effects=True, vmem_limit_bytes=56 * 1024 * 1024
            ),
        )(x_blk, b_own, c_full, ridge_lam.reshape(1, 1))

    return jax.shard_map(
        local_sweeps,
        mesh=mesh,
        in_specs=(P("tube", "row", "col"), P(("col", "row", "tube"), None), P(None, None), P()),
        out_specs=(P(("row", "col", "tube"), None), P(("col", "row", "tube"), None), P(None, None)),
        check_vma=False,
    )
```

```python
import jax
import jax.numpy as jnp
from jax import lax
from jax.experimental import pallas as pl
from jax.experimental.pallas import tpu as pltpu
from jax.sharding import PartitionSpec as P

SWEEPS = 2
HI = lax.Precision.HIGHEST
MESH = pl.DeviceIdType.MESH
F32 = jnp.float32
BF16 = jnp.bfloat16

OFF_YZ = [(t, c, 0) for c in range(2) for t in range(2)][1:]
OFF_XZ = [(t, 0, w) for w in range(4) for t in range(2)][1:]
OFF_ALL_REST = [(t, c, w) for w in range(1, 4) for c in range(2) for t in range(2)]
OFF_ALL = OFF_YZ + OFF_ALL_REST


def dot_t0(a, b, **kw):
    return lax.dot_general(a, b, (((0,), (0,)), ((), ())), preferred_element_type=F32, **kw)


def kernel(
    x_hbm, b_ref, c_ref, lam_ref,
    a_out, b_out, c_out,
    xf, xh, u_ref, bcols, a16, at_ref, af, pa, rsa, vt, rsb, gbp, gbr, pc, cb,
    w_ref, e_ref, li_ref, inv_ref, ga_ref, gb_ref, cfac,
    x_sem, rsa_s, rsa_r, aga_s, aga_r, af_s, af_r, rsb_s, rsb_r, agb_s, agb_r, gb_s, gb_r, pc_s, pc_r,
):
    t = lax.axis_index("tube")
    c = lax.axis_index("col")
    w = lax.axis_index("row")
    kk, ii, jj = xf.shape
    rank = b_ref.shape[1]
    g = c * 2 + t
    q = w * 2 + t
    me = g * 4 + w

    for k in range(kk):
        pltpu.make_async_copy(x_hbm.at[k], xf.at[k], x_sem.at[k]).start()

    def dev(off):
        return ((t + off[0]) % 2, (c + off[1]) % 2, (w + off[2]) % 4)

    barrier = pltpu.get_barrier_semaphore()
    for off in OFF_ALL:
        pl.semaphore_signal(barrier, inc=1, device_id=dev(off), device_id_type=MESH)
    pl.semaphore_wait(barrier, len(OFF_ALL))

    def push(src, dst, ss, rs, off):
        return pltpu.make_async_remote_copy(
            src_ref=src, dst_ref=dst, send_sem=ss, recv_sem=rs, device_id=dev(off), device_id_type=MESH
        )

    def gather_b(s):
        return [
            push(bcols.at[s, q], bcols.at[s, q], agb_s.at[s, n], agb_r.at[s, n], off)
            for n, off in enumerate(OFF_XZ)
        ]

    def gram_copy(s):
        return push(gbp, gbr.at[s], gb_s.at[s], gb_r.at[s], (0, 1, 0))

    def u_pass(s):
        bmat = bcols[s].reshape(jj, rank)

        def body(k, _):
            u_ref[k] = jnp.dot(xh[k], bmat, preferred_element_type=F32)
            return 0

        lax.fori_loop(0, kk, body, 0)

    def start_gram_b(s):
        bmat = bcols[s].reshape(jj, rank)
        gbp[...] = dot_t0(bmat, bmat)
        gram_copy(s).start()

    def finish_gram_b(s):
        gram_copy(s).wait()
        gb_ref[...] = gbp[...] + gbr[s]

    def factor(gram_prod):
        rows = lax.broadcasted_iota(jnp.int32, (rank, rank), 0)
        cols = lax.broadcasted_iota(jnp.int32, (rank, rank), 1)
        eye = jnp.where(rows == cols, 1.0, 0.0).astype(F32)
        w_ref[:, :rank] = gram_prod + lam_ref[0, 0] * eye
        w_ref[:, rank:] = eye
        r1 = lax.broadcasted_iota(jnp.int32, (8, rank), 0)

        def lane(x, n):
            return jnp.take_along_axis(x, jnp.full((8, rank), n, jnp.int32), axis=1, mode="promise_in_bounds")

        def step(b, first):
            lo = pl.multiple_of(b * 8, 8)
            ps = w_ref[pl.ds(lo, 8), :rank]
            pi = w_ref[pl.ds(lo, 8), rank:]
            e = [lane(ps, lo + n) for n in range(8)]
            for n in range(8):
                for v in range(first, rank // 8):
                    e_ref[v, n] = lane(w_ref[8 * v : 8 * v + 8, :rank], lo + n)
            low = None
            piv = jnp.broadcast_to(e[0][0:1], (8, rank))
            for j in range(8):
                isq = lax.rsqrt(piv)
                rc = isq * isq
                if j < 7:
                    x = jnp.broadcast_to(e[j + 1][j : j + 1], (8, rank))
                    piv = jnp.broadcast_to(e[j + 1][j + 1 : j + 2], (8, rank)) - (x * x) * rc
                m = e[j] * rc
                hit = r1 == j
                pjs = jnp.broadcast_to(ps[j : j + 1], (8, rank))
                pji = jnp.broadcast_to(pi[j : j + 1], (8, rank))
                low = pji * isq if low is None else jnp.where(hit, pji * isq, low)
                ps = jnp.where(hit, pjs * rc, ps - m * pjs)
                pi = jnp.where(hit, pji * rc, pi - m * pji)
                for n in range(j + 1, 8):
                    en = jnp.broadcast_to(e[n][j : j + 1], (8, rank))
                    e[n] = jnp.where(hit, en * rc, e[n] - m * en)
            li_ref[pl.ds(lo, 8), :] = low
            qs = [jnp.broadcast_to(ps[n : n + 1], (8, rank)) for n in range(8)]
            qi = [jnp.broadcast_to(pi[n : n + 1], (8, rank)) for n in range(8)]
            for v in range(first, rank // 8):
                ds = [e_ref[v, n] * qs[n] for n in range(8)]
                di = [e_ref[v, n] * qi[n] for n in range(8)]
                while len(ds) > 1:
                    ds = [ds[n] + ds[n + 1] for n in range(0, len(ds), 2)]
                    di = [di[n] + di[n + 1] for n in range(0, len(di), 2)]
                w_ref[8 * v : 8 * v + 8, :rank] -= ds[0]
                w_ref[8 * v : 8 * v + 8, rank:] -= di[0]

        def run(lo, hi):
            def body(b, _):
                step(b, lo)
                return 0

            lax.fori_loop(lo, hi, body, 0)

        run(0, 8)
        run(8, 16)
        inv_ref[...] = dot_t0(li_ref[...], li_ref[...], precision=HI)

    bcols[0, q] = b_ref[...].astype(BF16)
    cps = gather_b(0)
    for cp in cps:
        cp.start()
    cfac[...] = c_ref[...]

    def load(k, _):
        pltpu.make_async_copy(x_hbm.at[k], xf.at[k], x_sem.at[k]).wait()
        xh[k] = xf[k].astype(BF16)
        return 0

    lax.fori_loop(0, kk, load, 0)
    for cp in cps:
        cp.wait()
    start_gram_b(0)
    u_pass(0)
    finish_gram_b(0)

    def sweep(s, _):
        c16 = cfac[...].astype(BF16)
        gram_c = dot_t0(c16, c16)

        def body_a(k, acc):
            return acc + u_ref[k] * cfac[pl.ds(t * kk + k, 1), :]

        part = lax.fori_loop(0, kk, body_a, jnp.zeros((ii, rank), F32))
        pa[...] = part.reshape(pa.shape)
        ra = []
        for n, off in enumerate(OFF_YZ):
            g2 = dev(off)[1] * 2 + dev(off)[0]
            ra.append(push(pa.at[g2], rsa.at[s, n], rsa_s.at[s, n], rsa_r.at[s, n], off))
        for cp in ra:
            cp.start()
        factor(gb_ref[...] * gram_c)
        for cp in ra:
            cp.wait()
        mtt_a = pa[g] + rsa[s, 0] + rsa[s, 1] + rsa[s, 2]
        a_own = jnp.dot(mtt_a, inv_ref[...], precision=HI, preferred_element_type=F32)
        a_out[...] = a_own
        a16[s, w, g] = a_own.astype(BF16)
        af[s, g] = a_own
        ga = [push(a16.at[s, w, g], a16.at[s, w, g], aga_s.at[s, n], aga_r.at[s, n], off) for n, off in enumerate(OFF_ALL)]
        for cp in ga:
            cp.start()
        fa = [push(af.at[s, g], af.at[s, g], af_s.at[s, n], af_r.at[s, n], off) for n, off in enumerate(OFF_YZ)]
        for cp in fa:
            cp.start()

        cmine = cfac[pl.ds(pl.multiple_of(t * kk, kk), kk), :]
        ct = jnp.transpose(jnp.concatenate([cmine, jnp.zeros((rank - kk, rank), F32)], axis=0))
        for k in range(kk):
            cb[k] = jnp.broadcast_to(ct[:, k : k + 1], (rank, rank))
        for cp in ga[:3]:
            cp.wait()
        at_ref[...] = jnp.transpose(a16[s, w].reshape(ii, rank))
        vt[...] = jnp.zeros_like(vt)

        def body_b(k, _):
            v = jnp.dot(at_ref[...], xh[k], preferred_element_type=F32)
            ck = cb[k]
            for n in range(jj // rank):
                vt[n] += v[:, n * rank : (n + 1) * rank] * ck
            return 0

        lax.fori_loop(0, kk, body_b, 0)
        rb = []
        for n, off in enumerate(OFF_XZ):
            q2 = dev(off)[2] * 2 + dev(off)[0]
            rb.append(push(vt.at[q2], rsb.at[s, n], rsb_s.at[s, n], rsb_r.at[s, n], off))
        for cp in rb:
            cp.start()
        for cp in ga[3:]:
            cp.wait()
        aall = a16[s].reshape(4 * ii, rank)
        ga_ref[...] = dot_t0(aall, aall)
        factor(ga_ref[...] * gram_c)
        for cp in rb:
            cp.wait()
        mtt_b = vt[q]
        for n in range(len(OFF_XZ)):
            mtt_b = mtt_b + rsb[s, n]
        b_own = jnp.transpose(jnp.dot(inv_ref[...], mtt_b, precision=HI, preferred_element_type=F32))
        b_out[...] = b_own
        bcols[s + 1, q] = b_own.astype(BF16)
        gcs = gather_b(s + 1)
        for cp in gcs:
            cp.start()
        for cp in gcs:
            cp.wait()

        start_gram_b(s + 1)
        u_pass(s + 1)
        for cp in fa:
            cp.wait()
        afull = af[s].reshape(ii, rank)
        pc[s, me] = jnp.concatenate(
            [jnp.sum(u_ref[k] * afull, axis=0, keepdims=True) for k in range(kk)], axis=0
        )
        cs = [push(pc.at[s, me], pc.at[s, me], pc_s.at[s, n], pc_r.at[s, n], off) for n, off in enumerate(OFF_ALL)]
        for cp in cs:
            cp.start()
        finish_gram_b(s + 1)
        factor(ga_ref[...] * gb_ref[...])
        for cp in cs:
            cp.wait()
        halves = []
        for t2 in range(2):
            tot = None
            for c2 in range(2):
                for w2 in range(4):
                    term = pc[s, (c2 * 2 + t2) * 4 + w2]
                    tot = term if tot is None else tot + term
            halves.append(tot)
        cfac[...] = jnp.dot(jnp.concatenate(halves, axis=0), inv_ref[...], precision=HI, preferred_element_type=F32)
        return 0

    lax.fori_loop(0, SWEEPS, sweep, 0)
    c_out[...] = cfac[...]


def solution(mesh):
    def local_sweeps(x_blk, b_own, c_full, ridge_lam):
        kk, ii, jj = x_blk.shape
        rank = b_own.shape[1]
        arows, brows = ii // 4, b_own.shape[0]
        dma = pltpu.SemaphoreType.DMA
        vmem = pl.BlockSpec(memory_space=pltpu.VMEM)
        return pl.pallas_call(
            kernel,
            name="als",
            out_shape=(
                jax.ShapeDtypeStruct((arows, rank), F32),
                jax.ShapeDtypeStruct((brows, rank), F32),
                jax.ShapeDtypeStruct(c_full.shape, F32),
            ),
            in_specs=[
                pl.BlockSpec(memory_space=pl.ANY), vmem, vmem, pl.BlockSpec(memory_space=pltpu.SMEM),
            ],
            out_specs=(vmem, vmem, vmem),
            scratch_shapes=[
                pltpu.VMEM((kk, ii, jj), F32),
                pltpu.VMEM((kk, ii, jj), BF16),
                pltpu.VMEM((kk, ii, rank), F32),
                pltpu.VMEM((SWEEPS + 1, 8, brows, rank), BF16),
                pltpu.VMEM((SWEEPS, 4, 4, arows, rank), BF16),
                pltpu.VMEM((rank, ii), BF16),
                pltpu.VMEM((SWEEPS, 4, arows, rank), F32),
                pltpu.VMEM((4, arows, rank), F32),
                pltpu.VMEM((SWEEPS, 3, arows, rank), F32),
                pltpu.VMEM((8, rank, brows), F32),
                pltpu.VMEM((SWEEPS, 7, rank, brows), F32),
                pltpu.VMEM((rank, rank), F32),
                pltpu.VMEM((SWEEPS + 1, rank, rank), F32),
                pltpu.VMEM((SWEEPS, 16, kk, rank), F32),
                pltpu.VMEM((kk, rank, rank), F32),
                pltpu.VMEM((rank, 2 * rank), F32),
                pltpu.VMEM((rank // 8, 8, 8, rank), F32),
                pltpu.VMEM((rank, rank), F32),
                pltpu.VMEM((rank, rank), F32),
                pltpu.VMEM((rank, rank), F32),
                pltpu.VMEM((rank, rank), F32),
                pltpu.VMEM(c_full.shape, F32),
                dma((kk,)),
                dma((SWEEPS, 3)), dma((SWEEPS, 3)),
                dma((SWEEPS, 15)), dma((SWEEPS, 15)),
                dma((SWEEPS, 3)), dma((SWEEPS, 3)),
                dma((SWEEPS, 7)), dma((SWEEPS, 7)),
                dma((SWEEPS + 1, 7)), dma((SWEEPS + 1, 7)),
                dma((SWEEPS + 1,)), dma((SWEEPS + 1,)),
                dma((SWEEPS, 15)), dma((SWEEPS, 15)),
            ],
            compiler_params=pltpu.CompilerParams(
                collective_id=0, has_side_effects=True, vmem_limit_bytes=56 * 1024 * 1024
            ),
        )(x_blk, b_own, c_full, ridge_lam.reshape(1, 1))

    return jax.shard_map(
        local_sweeps,
        mesh=mesh,
        in_specs=(P("tube", "row", "col"), P(("col", "row", "tube"), None), P(None, None), P()),
        out_specs=(P(("row", "col", "tube"), None), P(("col", "row", "tube"), None), P(None, None)),
        check_vma=False,
    )
```

```python
import jax
import jax.numpy as jnp
from jax import lax
from jax.experimental import pallas as pl
from jax.experimental.pallas import tpu as pltpu
from jax.sharding import PartitionSpec as P

SWEEPS = 2
HI = lax.Precision.HIGHEST
MESH = pl.DeviceIdType.MESH
F32 = jnp.float32
BF16 = jnp.bfloat16

YZ = [(1, 1, 0, 0), (0, 1, 0, 0), (1, 0, 0, 0)]
NEAR = [(1, 0, 0, 1), (1, 0, 0, 0), (0, 0, 0, 1)]
FAR = [(1, 0, 1, 1), (1, 0, 1, 0), (0, 0, 1, 1), (0, 0, 1, 0)]
ALL = YZ + [(t, c, x, k) for x, k in ((1, 1), (1, 0), (0, 1)) for c in (1, 0) for t in (1, 0)]


def dot_t0(a, b, **kw):
    return lax.dot_general(a, b, (((0,), (0,)), ((), ())), preferred_element_type=F32, **kw)


def kernel(
    x_hbm, b_hbm, c_hbm, lam_ref,
    out,
    xf, xh, u_ref, b_in, bcols, a16, at_ref, af, pa, rsa, vp, vpr, vo, rsb, gbp, gbr, pc, cb,
    w_ref, e_ref, li_ref, inv_ref, ga_ref, gb_ref, cfac,
    x_sem, in_sem, rsa_s, rsa_r, aga_s, aga_r, af_s, af_r, vp_s, vp_r, rsb_s, rsb_r, agb_s, agb_r, gb_s, gb_r, pc_s, pc_r,
):
    t = lax.axis_index("tube")
    c = lax.axis_index("col")
    w = lax.axis_index("row")
    xc, core = w // 2, w % 2
    kk, ii, jj = xf.shape
    rank = b_in.shape[1]
    g = c * 2 + t
    me = g * 4 + w

    ins = [
        pltpu.make_async_copy(b_hbm, b_in, in_sem.at[0]),
        pltpu.make_async_copy(c_hbm, cfac, in_sem.at[1]),
    ]
    for cp in ins:
        cp.start()
    depth = 4
    for k in range(depth):
        pltpu.make_async_copy(x_hbm.at[k], xf.at[k], x_sem.at[k]).start()

    def load(k, _):
        pltpu.make_async_copy(x_hbm.at[k], xf.at[k], x_sem.at[k]).wait()

        @pl.when(k + depth < kk)
        def _():
            pltpu.make_async_copy(x_hbm.at[k + depth], xf.at[k + depth], x_sem.at[k + depth]).start()

        for n in range(jj // ii):
            xh[k, n] = xf[k, :, n * ii : (n + 1) * ii].astype(BF16)
        return 0

    def dev(off):
        return ((t + off[0]) % 2, (c + off[1]) % 2, ((xc + off[2]) % 2) * 2 + (core + off[3]) % 2)

    barrier = pltpu.get_barrier_semaphore()
    for off in reversed(ALL):
        pl.semaphore_signal(barrier, inc=1, device_id=dev(off), device_id_type=MESH)
    for cp in ins:
        cp.wait()
    bcols[0, w, t] = b_in[...].astype(BF16)
    first = 4
    lax.fori_loop(0, first, load, 0)
    pl.semaphore_wait(barrier, len(ALL))

    def push(src, dst, ss, rs, off):
        return pltpu.make_async_remote_copy(
            src_ref=src, dst_ref=dst, send_sem=ss, recv_sem=rs, device_id=dev(off), device_id_type=MESH
        )

    def gather_b(s):
        return [
            push(bcols.at[s, w, t], bcols.at[s, w, t], agb_s.at[s, n], agb_r.at[s, n], off)
            for n, off in enumerate(NEAR + FAR)
        ]

    def gram_copy(s):
        return push(gbp, gbr.at[s], gb_s.at[s], gb_r.at[s], (0, 1, 0, 0))

    def half_u(s, x2, first):
        def body(k, _):
            acc = None if first else u_ref[k]
            for n in range(2):
                p = jnp.dot(
                    xh[k, x2 * 2 + n], bcols[s, x2 * 2 + n].reshape(2 * rank, rank), preferred_element_type=F32
                )
                acc = p if acc is None else acc + p
            u_ref[k] = acc
            return 0

        lax.fori_loop(0, kk, body, 0, unroll=8)

    def gather_and_u(s, cps):
        for cp in cps[:3]:
            cp.wait()
        half_u(s, xc, True)
        for cp in cps[3:]:
            cp.wait()
        bmat = bcols[s].reshape(jj, rank)
        gbp[...] = dot_t0(bmat, bmat)
        gram_copy(s).start()
        half_u(s, 1 - xc, False)

    def finish_gram_b(s):
        gram_copy(s).wait()
        gb_ref[...] = gbp[...] + gbr[s]

    def factor(gram_prod):
        rows = lax.broadcasted_iota(jnp.int32, (rank, rank), 0)
        cols = lax.broadcasted_iota(jnp.int32, (rank, rank), 1)
        eye = jnp.where(rows == cols, 1.0, 0.0).astype(F32)
        w_ref[:, :rank] = gram_prod + lam_ref[0, 0] * eye
        w_ref[:, rank:] = eye
        r1 = lax.broadcasted_iota(jnp.int32, (8, rank), 0)

        def lane(x, n):
            return jnp.take_along_axis(x, jnp.full((8, rank), n, jnp.int32), axis=1, mode="promise_in_bounds")

        def step(b, first):
            lo = pl.multiple_of(b * 8, 8)
            ps = w_ref[pl.ds(lo, 8), :rank]
            pi = w_ref[pl.ds(lo, 8), rank:]
            e = [lane(ps, lo + n) for n in range(8)]
            for n in range(8):
                for v in range(first, rank // 8):
                    e_ref[v, n] = lane(w_ref[8 * v : 8 * v + 8, :rank], lo + n)
            low = None
            piv = jnp.broadcast_to(e[0][0:1], (8, rank))
            for j in range(8):
                isq = lax.rsqrt(piv)
                rc = isq * isq
                if j < 7:
                    x = jnp.broadcast_to(e[j + 1][j : j + 1], (8, rank))
                    piv = jnp.broadcast_to(e[j + 1][j + 1 : j + 2], (8, rank)) - (x * x) * rc
                m = e[j] * rc
                hit = r1 == j
                pjs = jnp.broadcast_to(ps[j : j + 1], (8, rank))
                pji = jnp.broadcast_to(pi[j : j + 1], (8, rank))
                low = pji * isq if low is None else jnp.where(hit, pji * isq, low)
                ps = jnp.where(hit, pjs * rc, ps - m * pjs)
                pi = jnp.where(hit, pji * rc, pi - m * pji)
                for n in range(j + 1, 8):
                    en = jnp.broadcast_to(e[n][j : j + 1], (8, rank))
                    e[n] = jnp.where(hit, en * rc, e[n] - m * en)
            li_ref[pl.ds(lo, 8), :] = low
            qs = [jnp.broadcast_to(ps[n : n + 1], (8, rank)) for n in range(8)]
            qi = [jnp.broadcast_to(pi[n : n + 1], (8, rank)) for n in range(8)]
            for v in range(first, rank // 8):
                ds = [e_ref[v, n] * qs[n] for n in range(8)]
                di = [e_ref[v, n] * qi[n] for n in range(8)]
                while len(ds) > 1:
                    ds = [ds[n] + ds[n + 1] for n in range(0, len(ds), 2)]
                    di = [di[n] + di[n + 1] for n in range(0, len(di), 2)]
                w_ref[8 * v : 8 * v + 8, :rank] -= ds[0]
                w_ref[8 * v : 8 * v + 8, rank:] -= di[0]

        def run(lo, hi):
            def body(b, _):
                step(b, lo)
                return 0

            lax.fori_loop(lo, hi, body, 0)

        run(0, 8)
        run(8, 16)
        inv_ref[...] = dot_t0(li_ref[...], li_ref[...], precision=HI)

    cps = gather_b(0)
    for cp in cps:
        cp.start()

    lax.fori_loop(first, kk, load, 0)
    gather_and_u(0, cps)
    finish_gram_b(0)

    def sweep(s, _):
        c16 = cfac[...].astype(BF16)
        gram_c = dot_t0(c16, c16)

        def body_a(k, acc):
            return acc + u_ref[k] * cfac[pl.ds(t * kk + k, 1), :]

        part = lax.fori_loop(0, kk, body_a, jnp.zeros((ii, rank), F32))
        pa[...] = part.reshape(pa.shape)
        ra = []
        for n, off in enumerate(YZ):
            g2 = dev(off)[1] * 2 + dev(off)[0]
            ra.append(push(pa.at[g2], rsa.at[s, n], rsa_s.at[s, n], rsa_r.at[s, n], off))
        for cp in ra:
            cp.start()
        factor(gb_ref[...] * gram_c)
        for cp in ra:
            cp.wait()
        mtt_a = pa[g] + rsa[s, 0] + rsa[s, 1] + rsa[s, 2]
        a_own = jnp.dot(mtt_a, inv_ref[...], precision=HI, preferred_element_type=F32)
        a16[s, w, g] = a_own.astype(BF16)
        af[s, g] = a_own
        ga = [push(a16.at[s, w, g], a16.at[s, w, g], aga_s.at[s, n], aga_r.at[s, n], off) for n, off in enumerate(ALL)]
        for cp in ga:
            cp.start()
        fa = [push(af.at[s, g], af.at[s, g], af_s.at[s, n], af_r.at[s, n], off) for n, off in enumerate(YZ)]
        for cp in fa:
            cp.start()
        out[: a_own.shape[0], :] = a_own

        cmine = cfac[pl.ds(pl.multiple_of(t * kk, kk), kk), :]
        ct = jnp.transpose(jnp.concatenate([cmine, jnp.zeros((rank - kk, rank), F32)], axis=0))
        for k in range(kk):
            cb[k] = jnp.broadcast_to(ct[:, k : k + 1], (rank, rank))
        for cp in ga[:3]:
            cp.wait()
        at_ref[...] = jnp.transpose(a16[s, w].reshape(ii, rank))

        def chunk(wc):
            def body(k, acc):
                ck = cb[k]
                return acc + jnp.dot(at_ref[...], xh[k, wc], preferred_element_type=F32) * jnp.concatenate([ck, ck], axis=1)

            return lax.fori_loop(0, kk, body, jnp.zeros((rank, ii), F32), unroll=16)

        vc = []
        for n in range(2):
            vp[n] = chunk(((xc + 1 - n) % 2) * 2 + (1 - core))
            vc.append(push(vp.at[n], vpr.at[s, n], vp_s.at[s, n], vp_r.at[s, n], (0, 0, 0, 1)))
            vc[n].start()
        rb = []
        for n in range(2):
            mine = chunk(((xc + 1 - n) % 2) * 2 + core)
            vc[n].wait()
            mine = mine + vpr[s, n]
            vo[n, 0] = mine[:, :rank]
            vo[n, 1] = mine[:, rank:]
            for off in ((1, 0, 1, 0), (0, 0, 1, 0)) if n == 0 else ((1, 0, 0, 0),):
                m = len(rb)
                rb.append(push(vo.at[n, dev(off)[0]], rsb.at[s, m], rsb_s.at[s, m], rsb_r.at[s, m], off))
                rb[m].start()
        for cp in ga[3:]:
            cp.wait()
        aall = a16[s].reshape(4 * ii, rank)
        ga_ref[...] = dot_t0(aall, aall)
        factor(ga_ref[...] * gram_c)
        for cp in rb:
            cp.wait()
        mtt_b = vo[1, t] + rsb[s, 0] + rsb[s, 1] + rsb[s, 2]
        b_own = jnp.transpose(jnp.dot(inv_ref[...], mtt_b, precision=HI, preferred_element_type=F32))
        bcols[s + 1, w, t] = b_own.astype(BF16)
        gcs = gather_b(s + 1)
        for cp in gcs:
            cp.start()
        out[ii // 4 : ii // 4 + rank, :] = b_own

        gather_and_u(s + 1, gcs)
        for cp in fa:
            cp.wait()
        afull = af[s].reshape(ii, rank)
        pc[s, me] = jnp.concatenate(
            [jnp.sum(u_ref[k] * afull, axis=0, keepdims=True) for k in range(kk)], axis=0
        )
        cs = [push(pc.at[s, me], pc.at[s, me], pc_s.at[s, n], pc_r.at[s, n], off) for n, off in enumerate(ALL)]
        for cp in cs:
            cp.start()
        finish_gram_b(s + 1)
        factor(ga_ref[...] * gb_ref[...])
        for cp in cs:
            cp.wait()
        halves = []
        for t2 in range(2):
            tot = None
            for c2 in range(2):
                for w2 in range(4):
                    term = pc[s, (c2 * 2 + t2) * 4 + w2]
                    tot = term if tot is None else tot + term
            halves.append(tot)
        cfac[...] = jnp.dot(jnp.concatenate(halves, axis=0), inv_ref[...], precision=HI, preferred_element_type=F32)
        return 0

    lax.fori_loop(0, SWEEPS, sweep, 0)
    out[ii // 4 + rank :, :] = cfac[...]


def split(rows, packed):
    def copy(src, *dsts):
        at = 0
        for n, dst in zip(rows, dsts):
            dst[...] = src[at : at + n, :]
            at += n

    vmem = pl.BlockSpec(memory_space=pltpu.VMEM)
    return pl.pallas_call(
        copy,
        name="results",
        out_shape=tuple(jax.ShapeDtypeStruct((n, packed.shape[1]), packed.dtype) for n in rows),
        in_specs=[vmem],
        out_specs=(vmem,) * len(rows),
        compiler_params=pltpu.CompilerParams(vmem_limit_bytes=1024 * 1024),
    )(packed)


def solution(mesh):
    def local_sweeps(x_blk, b_own, c_full, ridge_lam):
        kk, ii, jj = x_blk.shape
        brows, rank = b_own.shape
        arows, crows = ii // 4, c_full.shape[0]
        dma = pltpu.SemaphoreType.DMA
        vmem = pl.BlockSpec(memory_space=pltpu.VMEM)
        hbm = pl.BlockSpec(memory_space=pl.ANY)

        def sems(*shape):
            return [dma(shape), dma(shape)]

        packed = pl.pallas_call(
            kernel,
            name="als",
            out_shape=jax.ShapeDtypeStruct((arows + brows + crows, rank), F32),
            in_specs=[hbm, hbm, hbm, pl.BlockSpec(memory_space=pltpu.SMEM)],
            out_specs=vmem,
            scratch_shapes=[
                pltpu.VMEM((kk, ii, jj), F32),
                pltpu.VMEM((kk, jj // ii, ii, ii), BF16),
                pltpu.VMEM((kk, ii, rank), F32),
                pltpu.VMEM((brows, rank), F32),
                pltpu.VMEM((SWEEPS + 1, 4, 2, brows, rank), BF16),
                pltpu.VMEM((SWEEPS, 4, 4, arows, rank), BF16),
                pltpu.VMEM((rank, ii), BF16),
                pltpu.VMEM((SWEEPS, 4, arows, rank), F32),
                pltpu.VMEM((4, arows, rank), F32),
                pltpu.VMEM((SWEEPS, 3, arows, rank), F32),
                pltpu.VMEM((2, rank, 2 * brows), F32),
                pltpu.VMEM((SWEEPS, 2, rank, 2 * brows), F32),
                pltpu.VMEM((2, 2, rank, brows), F32),
                pltpu.VMEM((SWEEPS, 3, rank, brows), F32),
                pltpu.VMEM((rank, rank), F32),
                pltpu.VMEM((SWEEPS + 1, rank, rank), F32),
                pltpu.VMEM((SWEEPS, 16, kk, rank), F32),
                pltpu.VMEM((kk, rank, rank), F32),
                pltpu.VMEM((rank, 2 * rank), F32),
                pltpu.VMEM((rank // 8, 8, 8, rank), F32),
                pltpu.VMEM((rank, rank), F32),
                pltpu.VMEM((rank, rank), F32),
                pltpu.VMEM((rank, rank), F32),
                pltpu.VMEM((rank, rank), F32),
                pltpu.VMEM(c_full.shape, F32),
                dma((kk,)), dma((2,)),
                *sems(SWEEPS, 3), *sems(SWEEPS, 15), *sems(SWEEPS, 3), *sems(SWEEPS, 2), *sems(SWEEPS, 3),
                *sems(SWEEPS + 1, 7), *sems(SWEEPS + 1), *sems(SWEEPS, 15),
            ],
            compiler_params=pltpu.CompilerParams(
                collective_id=0, has_side_effects=True, vmem_limit_bytes=56 * 1024 * 1024
            ),
        )(x_blk, b_own, c_full, ridge_lam.reshape(1, 1))
        return split((arows, brows, crows), packed)

    return jax.shard_map(
        local_sweeps,
        mesh=mesh,
        in_specs=(P("tube", "row", "col"), P(("col", "row", "tube"), None), P(None, None), P()),
        out_specs=(P(("row", "col", "tube"), None), P(("col", "row", "tube"), None), P(None, None)),
        check_vma=False,
    )
```

```python
import jax
import jax.numpy as jnp
from jax import lax
from jax.experimental import pallas as pl
from jax.experimental.pallas import tpu as pltpu
from jax.sharding import PartitionSpec as P

SWEEPS = 2
HI = lax.Precision.HIGHEST
MESH = pl.DeviceIdType.MESH
F32 = jnp.float32
BF16 = jnp.bfloat16

YZ = [(1, 1, 0, 0), (0, 1, 0, 0), (1, 0, 0, 0)]
SAME_CORE = [(1, 0, 1, 0), (0, 0, 1, 0), (1, 0, 0, 0)]
PARTNER = (0, 0, 0, 1)
ALL = YZ + [(t, c, x, k) for x, k in ((1, 1), (1, 0), (0, 1)) for c in (1, 0) for t in (1, 0)]


def dot_t0(a, b, **kw):
    return lax.dot_general(a, b, (((0,), (0,)), ((), ())), preferred_element_type=F32, **kw)


def kernel(
    x_hbm, b_hbm, c_hbm, lam_ref,
    out,
    xf, xh, u_ref, b_in, bcols, a16, at_ref, af, pa, rsa, vp, vpr, vo, rsb, gbp, gbr, pc, cb,
    w_ref, e_ref, li_ref, inv_ref, ga_ref, gb_ref, cfac,
    x_sem, in_sem, rsa_s, rsa_r, aga_s, aga_r, af_s, af_r, vp_s, vp_r, rsb_s, rsb_r, agb_s, agb_r, gb_s, gb_r, pc_s, pc_r,
):
    t = lax.axis_index("tube")
    c = lax.axis_index("col")
    w = lax.axis_index("row")
    xc, core = w // 2, w % 2
    kk, ii, jj = xf.shape
    rank = b_in.shape[1]
    g = c * 2 + t
    me = g * 4 + w

    ins = [
        pltpu.make_async_copy(b_hbm, b_in, in_sem.at[0]),
        pltpu.make_async_copy(c_hbm, cfac, in_sem.at[1]),
    ]
    for cp in ins:
        cp.start()
    depth = 4
    for k in range(depth):
        pltpu.make_async_copy(x_hbm.at[k], xf.at[k], x_sem.at[k]).start()

    def load(k, _):
        pltpu.make_async_copy(x_hbm.at[k], xf.at[k], x_sem.at[k]).wait()

        @pl.when(k + depth < kk)
        def _():
            pltpu.make_async_copy(x_hbm.at[k + depth], xf.at[k + depth], x_sem.at[k + depth]).start()

        for n in range(jj // ii):
            xh[k, n] = xf[k, :, n * ii : (n + 1) * ii].astype(BF16)
        return 0

    def dev(off):
        return ((t + off[0]) % 2, (c + off[1]) % 2, ((xc + off[2]) % 2) * 2 + (core + off[3]) % 2)

    barrier = pltpu.get_barrier_semaphore()
    for off in reversed(ALL):
        pl.semaphore_signal(barrier, inc=1, device_id=dev(off), device_id_type=MESH)
    for cp in ins:
        cp.wait()
    bcols[0, w, t] = b_in[...].astype(BF16)
    first = 4
    lax.fori_loop(0, first, load, 0)
    pl.semaphore_wait(barrier, len(ALL))

    def push(src, dst, ss, rs, off):
        return pltpu.make_async_remote_copy(
            src_ref=src, dst_ref=dst, send_sem=ss, recv_sem=rs, device_id=dev(off), device_id_type=MESH
        )

    def b_copy(s, n, src, off):
        block = bcols.at[s, src[2], src[0]]
        return push(block, block, agb_s.at[s, n], agb_r.at[s, n], off)

    def gather_b(s):
        cps = [b_copy(s, n, (t, c, w), off) for n, off in enumerate(SAME_CORE + [PARTNER])]
        for cp in cps:
            cp.start()
        return cps

    def relay_b(s, cps):
        fwd = []
        for n, off in reversed(list(enumerate(SAME_CORE))):
            cps[n].wait()
            fwd.append(b_copy(s, 4 + n, dev(off), PARTNER))
            fwd[-1].start()
        cps[3].wait()
        for cp in fwd:
            cp.wait()

    def gram_copy(s):
        return push(gbp, gbr.at[s], gb_s.at[s], gb_r.at[s], (0, 1, 0, 0))

    def gather_and_u(s, cps):
        relay_b(s, cps)
        bmat = bcols[s].reshape(jj, rank)
        gbp[...] = dot_t0(bmat, bmat)
        gram_copy(s).start()

        def body(k, _):
            acc = None
            for n in range(4):
                p = jnp.dot(xh[k, n], bcols[s, n].reshape(2 * rank, rank), preferred_element_type=F32)
                acc = p if acc is None else acc + p
            u_ref[k] = acc
            return 0

        lax.fori_loop(0, kk, body, 0, unroll=4)

    def finish_gram_b(s):
        gram_copy(s).wait()
        gb_ref[...] = gbp[...] + gbr[s]

    def factor(gram_prod):
        rows = lax.broadcasted_iota(jnp.int32, (rank, rank), 0)
        cols = lax.broadcasted_iota(jnp.int32, (rank, rank), 1)
        eye = jnp.where(rows == cols, 1.0, 0.0).astype(F32)
        w_ref[:, :rank] = gram_prod + lam_ref[0, 0] * eye
        w_ref[:, rank:] = eye
        r1 = lax.broadcasted_iota(jnp.int32, (8, rank), 0)

        def lane(x, n):
            return jnp.take_along_axis(x, jnp.full((8, rank), n, jnp.int32), axis=1, mode="promise_in_bounds")

        def spread(x, n):
            return jnp.broadcast_to(x[n : n + 1], (8, rank))

        def step(b, first, last):
            lo = pl.multiple_of(b * 8, 8)
            ps = w_ref[pl.ds(lo, 8), :rank]
            pi = w_ref[pl.ds(lo, 8), rank:]
            e = [lane(ps, lo + n) for n in range(8)]
            for n in range(8):
                for v in range(first, last):
                    e_ref[v, n] = lane(w_ref[8 * v : 8 * v + 8, :rank], lo + n)
            low_s = low_i = None
            piv = spread(e[0], 0)
            for j in range(8):
                isq = lax.rsqrt(piv)
                rc = isq * isq
                if j < 7:
                    x = spread(e[j + 1], j)
                    piv = spread(e[j + 1], j + 1) - (x * x) * rc
                m = e[j] * rc
                hit = r1 == j
                pjs = spread(ps, j)
                pji = spread(pi, j)
                low_s = pjs * isq if low_s is None else jnp.where(hit, pjs * isq, low_s)
                low_i = pji * isq if low_i is None else jnp.where(hit, pji * isq, low_i)
                ps = jnp.where(hit, pjs * rc, ps - m * pjs)
                pi = jnp.where(hit, pji * rc, pi - m * pji)
                for n in range(j + 1, 8):
                    en = spread(e[n], j)
                    e[n] = jnp.where(hit, en * rc, e[n] - m * en)
            li_ref[pl.ds(lo, 8), :rank] = low_s
            li_ref[pl.ds(lo, 8), rank:] = low_i
            qs = [spread(ps, n) for n in range(8)]
            qi = [spread(pi, n) for n in range(8)]
            for v in range(first, last):
                ds = [e_ref[v, n] * qs[n] for n in range(8)]
                di = [e_ref[v, n] * qi[n] for n in range(8)]
                while len(ds) > 1:
                    ds = [ds[n] + ds[n + 1] for n in range(0, len(ds), 2)]
                    di = [di[n] + di[n + 1] for n in range(0, len(di), 2)]
                w_ref[8 * v : 8 * v + 8, :rank] -= ds[0]
                w_ref[8 * v : 8 * v + 8, rank:] -= di[0]

        def run(lo, hi, first, last):
            def body(b, _):
                step(b, first, last)
                return 0

            lax.fori_loop(lo, hi, body, 0)

        half, end = rank // 16, rank // 8
        mid = rank // 2
        run(0, half // 2, 0, half)
        run(half // 2, half, half // 2, half)
        w_ref[mid:, :] = w_ref[mid:, :] - dot_t0(li_ref[:mid, mid:rank], li_ref[:mid, :], precision=HI)
        run(half, half + half // 2, half, end)
        run(half + half // 2, end, half + half // 2, end)
        inv_ref[...] = dot_t0(li_ref[:, rank:], li_ref[:, rank:], precision=HI)

    cps = gather_b(0)

    lax.fori_loop(first, kk, load, 0)
    gather_and_u(0, cps)
    finish_gram_b(0)

    def sweep(s, _):
        c16 = cfac[...].astype(BF16)
        gram_c = dot_t0(c16, c16)

        def body_a(k, acc):
            return acc + u_ref[k] * cfac[pl.ds(t * kk + k, 1), :]

        part = lax.fori_loop(0, kk, body_a, jnp.zeros((ii, rank), F32))
        pa[...] = part.reshape(pa.shape)
        ra = []
        for n, off in enumerate(YZ):
            g2 = dev(off)[1] * 2 + dev(off)[0]
            ra.append(push(pa.at[g2], rsa.at[s, n], rsa_s.at[s, n], rsa_r.at[s, n], off))
        for cp in ra:
            cp.start()
        factor(gb_ref[...] * gram_c)
        for cp in ra:
            cp.wait()
        mtt_a = pa[g] + rsa[s, 0] + rsa[s, 1] + rsa[s, 2]
        a_own = jnp.dot(mtt_a, inv_ref[...], precision=HI, preferred_element_type=F32)
        a16[s, w, g] = a_own.astype(BF16)
        af[s, g] = a_own
        ga = [push(a16.at[s, w, g], a16.at[s, w, g], aga_s.at[s, n], aga_r.at[s, n], off) for n, off in enumerate(ALL)]
        for cp in ga:
            cp.start()
        fa = [push(af.at[s, g], af.at[s, g], af_s.at[s, n], af_r.at[s, n], off) for n, off in enumerate(YZ)]
        for cp in fa:
            cp.start()
        out[: a_own.shape[0], :] = a_own

        cmine = cfac[pl.ds(pl.multiple_of(t * kk, kk), kk), :]
        ct = jnp.transpose(jnp.concatenate([cmine, jnp.zeros((rank - kk, rank), F32)], axis=0))
        for k in range(kk):
            cb[k] = jnp.broadcast_to(ct[:, k : k + 1], (rank, rank))
        for cp in ga[:3]:
            cp.wait()
        at_ref[...] = jnp.transpose(a16[s, w].reshape(ii, rank))

        def chunk(wc):
            def body(k, acc):
                ck = cb[k]
                return acc + jnp.dot(at_ref[...], xh[k, wc], preferred_element_type=F32) * jnp.concatenate([ck, ck], axis=1)

            return lax.fori_loop(0, kk, body, jnp.zeros((rank, ii), F32), unroll=16)

        vc = []
        for n in range(2):
            vp[n] = chunk(((xc + 1 - n) % 2) * 2 + (1 - core))
            vc.append(push(vp.at[n], vpr.at[s, n], vp_s.at[s, n], vp_r.at[s, n], (0, 0, 0, 1)))
            vc[n].start()
        rb = []
        for n in range(2):
            mine = chunk(((xc + 1 - n) % 2) * 2 + core)
            vc[n].wait()
            mine = mine + vpr[s, n]
            vo[n, 0] = mine[:, :rank]
            vo[n, 1] = mine[:, rank:]
            for off in ((1, 0, 1, 0), (0, 0, 1, 0)) if n == 0 else ((1, 0, 0, 0),):
                m = len(rb)
                rb.append(push(vo.at[n, dev(off)[0]], rsb.at[s, m], rsb_s.at[s, m], rsb_r.at[s, m], off))
                rb[m].start()
        for cp in ga[3:]:
            cp.wait()
        aall = a16[s].reshape(4 * ii, rank)
        ga_ref[...] = dot_t0(aall, aall)
        factor(ga_ref[...] * gram_c)
        for cp in rb:
            cp.wait()
        mtt_b = vo[1, t] + rsb[s, 0] + rsb[s, 1] + rsb[s, 2]
        b_own = jnp.transpose(jnp.dot(inv_ref[...], mtt_b, precision=HI, preferred_element_type=F32))
        bcols[s + 1, w, t] = b_own.astype(BF16)
        gcs = gather_b(s + 1)
        out[ii // 4 : ii // 4 + rank, :] = b_own

        gather_and_u(s + 1, gcs)
        for cp in fa:
            cp.wait()
        afull = af[s].reshape(ii, rank)
        pc[s, me] = jnp.concatenate(
            [jnp.sum(u_ref[k] * afull, axis=0, keepdims=True) for k in range(kk)], axis=0
        )
        cs = [push(pc.at[s, me], pc.at[s, me], pc_s.at[s, n], pc_r.at[s, n], off) for n, off in enumerate(ALL)]
        for cp in cs:
            cp.start()
        finish_gram_b(s + 1)
        factor(ga_ref[...] * gb_ref[...])
        for cp in cs:
            cp.wait()
        halves = []
        for t2 in range(2):
            tot = None
            for c2 in range(2):
                for w2 in range(4):
                    term = pc[s, (c2 * 2 + t2) * 4 + w2]
                    tot = term if tot is None else tot + term
            halves.append(tot)
        cfac[...] = jnp.dot(jnp.concatenate(halves, axis=0), inv_ref[...], precision=HI, preferred_element_type=F32)
        return 0

    lax.fori_loop(0, SWEEPS, sweep, 0)
    out[ii // 4 + rank :, :] = cfac[...]


def split(rows, packed):
    def copy(src, *dsts):
        at = 0
        for n, dst in zip(rows, dsts):
            dst[...] = src[at : at + n, :]
            at += n

    vmem = pl.BlockSpec(memory_space=pltpu.VMEM)
    return pl.pallas_call(
        copy,
        name="results",
        out_shape=tuple(jax.ShapeDtypeStruct((n, packed.shape[1]), packed.dtype) for n in rows),
        in_specs=[vmem],
        out_specs=(vmem,) * len(rows),
        compiler_params=pltpu.CompilerParams(vmem_limit_bytes=1024 * 1024),
    )(packed)


def solution(mesh):
    def local_sweeps(x_blk, b_own, c_full, ridge_lam):
        kk, ii, jj = x_blk.shape
        brows, rank = b_own.shape
        arows, crows = ii // 4, c_full.shape[0]
        dma = pltpu.SemaphoreType.DMA
        vmem = pl.BlockSpec(memory_space=pltpu.VMEM)
        hbm = pl.BlockSpec(memory_space=pl.ANY)

        def sems(*shape):
            return [dma(shape), dma(shape)]

        packed = pl.pallas_call(
            kernel,
            name="als",
            out_shape=jax.ShapeDtypeStruct((arows + brows + crows, rank), F32),
            in_specs=[hbm, hbm, hbm, pl.BlockSpec(memory_space=pltpu.SMEM)],
            out_specs=vmem,
            scratch_shapes=[
                pltpu.VMEM((kk, ii, jj), F32),
                pltpu.VMEM((kk, jj // ii, ii, ii), BF16),
                pltpu.VMEM((kk, ii, rank), F32),
                pltpu.VMEM((brows, rank), F32),
                pltpu.VMEM((SWEEPS + 1, 4, 2, brows, rank), BF16),
                pltpu.VMEM((SWEEPS, 4, 4, arows, rank), BF16),
                pltpu.VMEM((rank, ii), BF16),
                pltpu.VMEM((SWEEPS, 4, arows, rank), F32),
                pltpu.VMEM((4, arows, rank), F32),
                pltpu.VMEM((SWEEPS, 3, arows, rank), F32),
                pltpu.VMEM((2, rank, 2 * brows), F32),
                pltpu.VMEM((SWEEPS, 2, rank, 2 * brows), F32),
                pltpu.VMEM((2, 2, rank, brows), F32),
                pltpu.VMEM((SWEEPS, 3, rank, brows), F32),
                pltpu.VMEM((rank, rank), F32),
                pltpu.VMEM((SWEEPS + 1, rank, rank), F32),
                pltpu.VMEM((SWEEPS, 16, kk, rank), F32),
                pltpu.VMEM((kk, rank, rank), F32),
                pltpu.VMEM((rank, 2 * rank), F32),
                pltpu.VMEM((rank // 8, 8, 8, rank), F32),
                pltpu.VMEM((rank, 2 * rank), F32),
                pltpu.VMEM((rank, rank), F32),
                pltpu.VMEM((rank, rank), F32),
                pltpu.VMEM((rank, rank), F32),
                pltpu.VMEM(c_full.shape, F32),
                dma((kk,)), dma((2,)),
                *sems(SWEEPS, 3), *sems(SWEEPS, 15), *sems(SWEEPS, 3), *sems(SWEEPS, 2), *sems(SWEEPS, 3),
                *sems(SWEEPS + 1, 7), *sems(SWEEPS + 1), *sems(SWEEPS, 15),
            ],
            compiler_params=pltpu.CompilerParams(
                collective_id=0, has_side_effects=True, vmem_limit_bytes=56 * 1024 * 1024
            ),
        )(x_blk, b_own, c_full, ridge_lam.reshape(1, 1))
        return split((arows, brows, crows), packed)

    return jax.shard_map(
        local_sweeps,
        mesh=mesh,
        in_specs=(P("tube", "row", "col"), P(("col", "row", "tube"), None), P(None, None), P()),
        out_specs=(P(("row", "col", "tube"), None), P(("col", "row", "tube"), None), P(None, None)),
        check_vma=False,
    )
```

```python
import jax
import jax.numpy as jnp
from jax import lax
from jax.experimental import pallas as pl
from jax.experimental.pallas import tpu as pltpu
from jax.sharding import PartitionSpec as P

SWEEPS = 2
HI = lax.Precision.HIGHEST
MESH = pl.DeviceIdType.MESH
F32 = jnp.float32
BF16 = jnp.bfloat16

YZ = [(1, 1, 0, 0), (0, 1, 0, 0), (1, 0, 0, 0)]
SAME_CORE = [(1, 0, 1, 0), (0, 0, 1, 0), (1, 0, 0, 0)]
YZ_FAR = [(1, 1, 1, 0), (0, 1, 1, 0), (1, 0, 1, 0), (0, 0, 1, 0)]
PARTNER = (0, 0, 0, 1)
ALL = YZ + [(t, c, x, k) for x, k in ((1, 1), (1, 0), (0, 1)) for c in (1, 0) for t in (1, 0)]


def dot_t0(a, b, **kw):
    return lax.dot_general(a, b, (((0,), (0,)), ((), ())), preferred_element_type=F32, **kw)


def kernel(
    x_hbm, b_hbm, c_hbm, lam_ref,
    out,
    xf, xh, u_ref, b_in, bcols, a16, at_ref, af, pa, rsa, vp, vpr, vo, rsb, gbp, gbr, pc, cb,
    w_ref, e_ref, li_ref, inv_ref, ga_ref, gb_ref, cfac,
    x_sem, in_sem, rsa_s, rsa_r, aga_s, aga_r, af_s, af_r, vp_s, vp_r, rsb_s, rsb_r, agb_s, agb_r, gb_s, gb_r, pc_s, pc_r,
):
    t = lax.axis_index("tube")
    c = lax.axis_index("col")
    w = lax.axis_index("row")
    xc, core = w // 2, w % 2
    kk, ii, jj = xf.shape
    rank = b_in.shape[1]
    g = c * 2 + t
    me = g * 4 + w

    ins = [
        pltpu.make_async_copy(b_hbm, b_in, in_sem.at[0]),
        pltpu.make_async_copy(c_hbm, cfac, in_sem.at[1]),
    ]
    for cp in ins:
        cp.start()
    depth = 4
    for k in range(depth):
        pltpu.make_async_copy(x_hbm.at[k], xf.at[k], x_sem.at[k]).start()

    def load(k, _):
        pltpu.make_async_copy(x_hbm.at[k], xf.at[k], x_sem.at[k]).wait()

        @pl.when(k + depth < kk)
        def _():
            pltpu.make_async_copy(x_hbm.at[k + depth], xf.at[k + depth], x_sem.at[k + depth]).start()

        for n in range(jj // ii):
            xh[k, n] = xf[k, :, n * ii : (n + 1) * ii].astype(BF16)
        return 0

    def dev(off):
        return ((t + off[0]) % 2, (c + off[1]) % 2, ((xc + off[2]) % 2) * 2 + (core + off[3]) % 2)

    barrier = pltpu.get_barrier_semaphore()
    for off in reversed(ALL):
        pl.semaphore_signal(barrier, inc=1, device_id=dev(off), device_id_type=MESH)
    for cp in ins:
        cp.wait()
    bcols[0, w, t] = b_in[...].astype(BF16)
    first = 4
    lax.fori_loop(0, first, load, 0)
    pl.semaphore_wait(barrier, len(ALL))

    def push(src, dst, ss, rs, off):
        return pltpu.make_async_remote_copy(
            src_ref=src, dst_ref=dst, send_sem=ss, recv_sem=rs, device_id=dev(off), device_id_type=MESH
        )

    def b_copy(s, n, src, off):
        block = bcols.at[s, src[2], src[0]]
        return push(block, block, agb_s.at[s, n], agb_r.at[s, n], off)

    def gather_b(s):
        cps = [b_copy(s, n, (t, c, w), off) for n, off in enumerate(SAME_CORE + [PARTNER])]
        for cp in cps:
            cp.start()
        return cps

    def relay_b(s, cps):
        fwd = []
        for n, off in reversed(list(enumerate(SAME_CORE))):
            cps[n].wait()
            fwd.append(b_copy(s, 4 + n, dev(off), PARTNER))
            fwd[-1].start()
        cps[3].wait()
        for cp in fwd:
            cp.wait()

    def gram_copy(s):
        return push(gbp, gbr.at[s], gb_s.at[s], gb_r.at[s], (0, 1, 0, 0))

    def gather_and_u(s, cps):
        relay_b(s, cps)
        bmat = bcols[s].reshape(jj, rank)
        gbp[...] = dot_t0(bmat, bmat)
        gram_copy(s).start()

        def body(k, _):
            acc = None
            for n in range(4):
                p = jnp.dot(xh[k, n], bcols[s, n].reshape(2 * rank, rank), preferred_element_type=F32)
                acc = p if acc is None else acc + p
            u_ref[k] = acc
            return 0

        lax.fori_loop(0, kk, body, 0, unroll=4)

    def finish_gram_b(s):
        gram_copy(s).wait()
        gb_ref[...] = gbp[...] + gbr[s]

    def factor(gram_prod):
        rows = lax.broadcasted_iota(jnp.int32, (rank, rank), 0)
        cols = lax.broadcasted_iota(jnp.int32, (rank, rank), 1)
        eye = jnp.where(rows == cols, 1.0, 0.0).astype(F32)
        w_ref[:, :rank] = gram_prod + lam_ref[0, 0] * eye
        w_ref[:, rank:] = eye
        r1 = lax.broadcasted_iota(jnp.int32, (8, rank), 0)

        def lane(x, n):
            return jnp.take_along_axis(x, jnp.full((8, rank), n, jnp.int32), axis=1, mode="promise_in_bounds")

        def spread(x, n):
            return jnp.broadcast_to(x[n : n + 1], (8, rank))

        def step(b, first, last):
            lo = pl.multiple_of(b * 8, 8)
            ps = w_ref[pl.ds(lo, 8), :rank]
            pi = w_ref[pl.ds(lo, 8), rank:]
            e = [lane(ps, lo + n) for n in range(8)]
            for n in range(8):
                for v in range(first, last):
                    e_ref[v, n] = lane(w_ref[8 * v : 8 * v + 8, :rank], lo + n)
            low_s = low_i = None
            piv = spread(e[0], 0)
            for j in range(8):
                isq = lax.rsqrt(piv)
                rc = isq * isq
                if j < 7:
                    x = spread(e[j + 1], j)
                    piv = spread(e[j + 1], j + 1) - (x * x) * rc
                m = e[j] * rc
                hit = r1 == j
                pjs = spread(ps, j)
                pji = spread(pi, j)
                low_s = pjs * isq if low_s is None else jnp.where(hit, pjs * isq, low_s)
                low_i = pji * isq if low_i is None else jnp.where(hit, pji * isq, low_i)
                ps = jnp.where(hit, pjs * rc, ps - m * pjs)
                pi = jnp.where(hit, pji * rc, pi - m * pji)
                for n in range(j + 1, 8):
                    en = spread(e[n], j)
                    e[n] = jnp.where(hit, en * rc, e[n] - m * en)
            li_ref[pl.ds(lo, 8), :rank] = low_s
            li_ref[pl.ds(lo, 8), rank:] = low_i
            qs = [spread(ps, n) for n in range(8)]
            qi = [spread(pi, n) for n in range(8)]
            for v in range(first, last):
                ds = [e_ref[v, n] * qs[n] for n in range(8)]
                di = [e_ref[v, n] * qi[n] for n in range(8)]
                while len(ds) > 1:
                    ds = [ds[n] + ds[n + 1] for n in range(0, len(ds), 2)]
                    di = [di[n] + di[n + 1] for n in range(0, len(di), 2)]
                w_ref[8 * v : 8 * v + 8, :rank] -= ds[0]
                w_ref[8 * v : 8 * v + 8, rank:] -= di[0]

        def run(lo, hi, first, last):
            def body(b, _):
                step(b, first, last)
                return 0

            lax.fori_loop(lo, hi, body, 0)

        half, end = rank // 16, rank // 8
        mid = rank // 2
        run(0, half // 2, 0, half)
        run(half // 2, half, half // 2, half)
        w_ref[mid:, :] = w_ref[mid:, :] - dot_t0(li_ref[:mid, mid:rank], li_ref[:mid, :], precision=HI)
        run(half, half + half // 2, half, end)
        run(half + half // 2, end, half + half // 2, end)
        inv_ref[...] = dot_t0(li_ref[:, rank:], li_ref[:, rank:], precision=HI)

    cps = gather_b(0)

    lax.fori_loop(first, kk, load, 0)
    gather_and_u(0, cps)
    finish_gram_b(0)

    def sweep(s, _):
        c16 = cfac[...].astype(BF16)
        gram_c = dot_t0(c16, c16)

        def body_a(k, acc):
            return acc + u_ref[k] * cfac[pl.ds(t * kk + k, 1), :]

        part = lax.fori_loop(0, kk, body_a, jnp.zeros((ii, rank), F32))
        pa[...] = part.reshape(pa.shape)
        ra = []
        for n, off in enumerate(YZ):
            g2 = dev(off)[1] * 2 + dev(off)[0]
            ra.append(push(pa.at[g2], rsa.at[s, n], rsa_s.at[s, n], rsa_r.at[s, n], off))
        for cp in ra:
            cp.start()
        factor(gb_ref[...] * gram_c)
        for cp in ra:
            cp.wait()
        mtt_a = pa[g] + rsa[s, 0] + rsa[s, 1] + rsa[s, 2]
        a_own = jnp.dot(mtt_a, inv_ref[...], precision=HI, preferred_element_type=F32)
        a16[s, w, g] = a_own.astype(BF16)
        af[s, g] = a_own
        ga = [
            push(a16.at[s, w, g], a16.at[s, w, g], aga_s.at[s, n], aga_r.at[s, n], off) for n, off in enumerate(YZ + YZ_FAR)
        ]
        for cp in ga:
            cp.start()
        out[: a_own.shape[0], :] = a_own

        cmine = cfac[pl.ds(pl.multiple_of(t * kk, kk), kk), :]
        ct = jnp.transpose(jnp.concatenate([cmine, jnp.zeros((rank - kk, rank), F32)], axis=0))
        for k in range(kk):
            cb[k] = jnp.broadcast_to(ct[:, k : k + 1], (rank, rank))
        for cp in ga[:3]:
            cp.wait()

        def hand_on(w2, n):
            return push(a16.at[s, w2], a16.at[s, w2], aga_s.at[s, n], aga_r.at[s, n], PARTNER)

        near = hand_on(w, 7)
        near.start()
        at_ref[...] = jnp.transpose(a16[s, w].reshape(ii, rank))

        def chunk(wc):
            def body(k, acc):
                ck = cb[k]
                return acc + jnp.dot(at_ref[...], xh[k, wc], preferred_element_type=F32) * jnp.concatenate([ck, ck], axis=1)

            return lax.fori_loop(0, kk, body, jnp.zeros((rank, ii), F32), unroll=16)

        vc = []
        for n in range(2):
            vp[n] = chunk(((xc + 1 - n) % 2) * 2 + (1 - core))
            vc.append(push(vp.at[n], vpr.at[s, n], vp_s.at[s, n], vp_r.at[s, n], (0, 0, 0, 1)))
            vc[n].start()
        for cp in ga[3:]:
            cp.wait()
        far = hand_on((1 - xc) * 2 + core, 8)
        far.start()
        rb = []
        for n in range(2):
            mine = chunk(((xc + 1 - n) % 2) * 2 + core)
            vc[n].wait()
            mine = mine + vpr[s, n]
            vo[n, 0] = mine[:, :rank]
            vo[n, 1] = mine[:, rank:]
            for off in ((1, 0, 1, 0), (0, 0, 1, 0)) if n == 0 else ((1, 0, 0, 0),):
                m = len(rb)
                rb.append(push(vo.at[n, dev(off)[0]], rsb.at[s, m], rsb_s.at[s, m], rsb_r.at[s, m], off))
                rb[m].start()
        fa = [push(af.at[s, g], af.at[s, g], af_s.at[s, n], af_r.at[s, n], off) for n, off in enumerate(YZ)]
        for cp in fa:
            cp.start()
        near.wait()
        far.wait()
        aall = a16[s].reshape(4 * ii, rank)
        ga_ref[...] = dot_t0(aall, aall)
        factor(ga_ref[...] * gram_c)
        for cp in rb:
            cp.wait()
        mtt_b = vo[1, t] + rsb[s, 0] + rsb[s, 1] + rsb[s, 2]
        b_own = jnp.transpose(jnp.dot(inv_ref[...], mtt_b, precision=HI, preferred_element_type=F32))
        bcols[s + 1, w, t] = b_own.astype(BF16)
        gcs = gather_b(s + 1)
        out[ii // 4 : ii // 4 + rank, :] = b_own

        gather_and_u(s + 1, gcs)
        for cp in fa:
            cp.wait()
        afull = af[s].reshape(ii, rank)
        pc[s, me] = jnp.concatenate(
            [jnp.sum(u_ref[k] * afull, axis=0, keepdims=True) for k in range(kk)], axis=0
        )
        cs = [push(pc.at[s, me], pc.at[s, me], pc_s.at[s, n], pc_r.at[s, n], off) for n, off in enumerate(ALL)]
        for cp in cs:
            cp.start()
        finish_gram_b(s + 1)
        factor(ga_ref[...] * gb_ref[...])
        for cp in cs:
            cp.wait()
        halves = []
        for t2 in range(2):
            tot = None
            for c2 in range(2):
                for w2 in range(4):
                    term = pc[s, (c2 * 2 + t2) * 4 + w2]
                    tot = term if tot is None else tot + term
            halves.append(tot)
        cfac[...] = jnp.dot(jnp.concatenate(halves, axis=0), inv_ref[...], precision=HI, preferred_element_type=F32)
        return 0

    lax.fori_loop(0, SWEEPS, sweep, 0)
    out[ii // 4 + rank :, :] = cfac[...]


def split(rows, packed):
    def copy(src, *dsts):
        at = 0
        for n, dst in zip(rows, dsts):
            dst[...] = src[at : at + n, :]
            at += n

    vmem = pl.BlockSpec(memory_space=pltpu.VMEM)
    return pl.pallas_call(
        copy,
        name="results",
        out_shape=tuple(jax.ShapeDtypeStruct((n, packed.shape[1]), packed.dtype) for n in rows),
        in_specs=[vmem],
        out_specs=(vmem,) * len(rows),
        compiler_params=pltpu.CompilerParams(vmem_limit_bytes=1024 * 1024),
    )(packed)


def solution(mesh):
    def local_sweeps(x_blk, b_own, c_full, ridge_lam):
        kk, ii, jj = x_blk.shape
        brows, rank = b_own.shape
        arows, crows = ii // 4, c_full.shape[0]
        dma = pltpu.SemaphoreType.DMA
        vmem = pl.BlockSpec(memory_space=pltpu.VMEM)
        hbm = pl.BlockSpec(memory_space=pl.ANY)

        def sems(*shape):
            return [dma(shape), dma(shape)]

        packed = pl.pallas_call(
            kernel,
            name="als",
            out_shape=jax.ShapeDtypeStruct((arows + brows + crows, rank), F32),
            in_specs=[hbm, hbm, hbm, pl.BlockSpec(memory_space=pltpu.SMEM)],
            out_specs=vmem,
            scratch_shapes=[
                pltpu.VMEM((kk, ii, jj), F32),
                pltpu.VMEM((kk, jj // ii, ii, ii), BF16),
                pltpu.VMEM((kk, ii, rank), F32),
                pltpu.VMEM((brows, rank), F32),
                pltpu.VMEM((SWEEPS + 1, 4, 2, brows, rank), BF16),
                pltpu.VMEM((SWEEPS, 4, 4, arows, rank), BF16),
                pltpu.VMEM((rank, ii), BF16),
                pltpu.VMEM((SWEEPS, 4, arows, rank), F32),
                pltpu.VMEM((4, arows, rank), F32),
                pltpu.VMEM((SWEEPS, 3, arows, rank), F32),
                pltpu.VMEM((2, rank, 2 * brows), F32),
                pltpu.VMEM((SWEEPS, 2, rank, 2 * brows), F32),
                pltpu.VMEM((2, 2, rank, brows), F32),
                pltpu.VMEM((SWEEPS, 3, rank, brows), F32),
                pltpu.VMEM((rank, rank), F32),
                pltpu.VMEM((SWEEPS + 1, rank, rank), F32),
                pltpu.VMEM((SWEEPS, 16, kk, rank), F32),
                pltpu.VMEM((kk, rank, rank), F32),
                pltpu.VMEM((rank, 2 * rank), F32),
                pltpu.VMEM((rank // 8, 8, 8, rank), F32),
                pltpu.VMEM((rank, 2 * rank), F32),
                pltpu.VMEM((rank, rank), F32),
                pltpu.VMEM((rank, rank), F32),
                pltpu.VMEM((rank, rank), F32),
                pltpu.VMEM(c_full.shape, F32),
                dma((kk,)), dma((2,)),
                *sems(SWEEPS, 3), *sems(SWEEPS, 9), *sems(SWEEPS, 3), *sems(SWEEPS, 2), *sems(SWEEPS, 3),
                *sems(SWEEPS + 1, 7), *sems(SWEEPS + 1), *sems(SWEEPS, 15),
            ],
            compiler_params=pltpu.CompilerParams(
                collective_id=0, has_side_effects=True, vmem_limit_bytes=56 * 1024 * 1024
            ),
        )(x_blk, b_own, c_full, ridge_lam.reshape(1, 1))
        return split((arows, brows, crows), packed)

    return jax.shard_map(
        local_sweeps,
        mesh=mesh,
        in_specs=(P("tube", "row", "col"), P(("col", "row", "tube"), None), P(None, None), P()),
        out_specs=(P(("row", "col", "tube"), None), P(("col", "row", "tube"), None), P(None, None)),
        check_vma=False,
    )
```

```python
import jax
import jax.numpy as jnp
from jax import lax
from jax.experimental import pallas as pl
from jax.experimental.pallas import tpu as pltpu
from jax.sharding import PartitionSpec as P

SWEEPS = 2
HI = lax.Precision.HIGHEST
MESH = pl.DeviceIdType.MESH
F32 = jnp.float32
BF16 = jnp.bfloat16

YZ = [(1, 1, 0, 0), (0, 1, 0, 0), (1, 0, 0, 0)]
SAME_CORE = [(1, 0, 1, 0), (0, 0, 1, 0), (1, 0, 0, 0)]
YZ_FAR = [(1, 1, 1, 0), (0, 1, 1, 0), (1, 0, 1, 0), (0, 0, 1, 0)]
PARTNER = (0, 0, 0, 1)
ALL = YZ + [(t, c, x, k) for x, k in ((1, 1), (1, 0), (0, 1)) for c in (1, 0) for t in (1, 0)]


def dot_t0(a, b, **kw):
    return lax.dot_general(a, b, (((0,), (0,)), ((), ())), preferred_element_type=F32, **kw)


def kernel(
    x_hbm, b_hbm, c_hbm, lam_ref,
    out,
    xf, xh, u_ref, b_in, bcols, a16, at_ref, af, pa, rsa, vp, vpr, vo, rsb, gbp, gbr, pc, cb,
    w_ref, e_ref, li_ref, inv_ref, ga_ref, gb_ref, cfac,
    x_sem, in_sem, rsa_s, rsa_r, aga_s, aga_r, af_s, af_r, vp_s, vp_r, rsb_s, rsb_r, agb_s, agb_r, gb_s, gb_r, pc_s, pc_r,
):
    t = lax.axis_index("tube")
    c = lax.axis_index("col")
    w = lax.axis_index("row")
    xc, core = w // 2, w % 2
    kk, ii, jj = xf.shape
    rank = b_in.shape[1]
    g = c * 2 + t
    me = g * 4 + w

    ins = [
        pltpu.make_async_copy(b_hbm, b_in, in_sem.at[0]),
        pltpu.make_async_copy(c_hbm, cfac, in_sem.at[1]),
    ]
    for cp in ins:
        cp.start()
    depth = 4
    for k in range(depth):
        pltpu.make_async_copy(x_hbm.at[k], xf.at[k], x_sem.at[k]).start()

    def load(k, _):
        pltpu.make_async_copy(x_hbm.at[k], xf.at[k], x_sem.at[k]).wait()

        @pl.when(k + depth < kk)
        def _():
            pltpu.make_async_copy(x_hbm.at[k + depth], xf.at[k + depth], x_sem.at[k + depth]).start()

        for n in range(jj // ii):
            xh[k, n] = xf[k, :, n * ii : (n + 1) * ii].astype(BF16)
        return 0

    def dev(off):
        return ((t + off[0]) % 2, (c + off[1]) % 2, ((xc + off[2]) % 2) * 2 + (core + off[3]) % 2)

    barrier = pltpu.get_barrier_semaphore()
    for off in reversed(ALL):
        pl.semaphore_signal(barrier, inc=1, device_id=dev(off), device_id_type=MESH)
    for cp in ins:
        cp.wait()
    bcols[0, w, t] = b_in[...].astype(BF16)
    first = 4
    lax.fori_loop(0, first, load, 0)
    pl.semaphore_wait(barrier, len(ALL))

    def push(src, dst, ss, rs, off):
        return pltpu.make_async_remote_copy(
            src_ref=src, dst_ref=dst, send_sem=ss, recv_sem=rs, device_id=dev(off), device_id_type=MESH
        )

    def b_copy(s, n, src, off):
        block = bcols.at[s, src[2], src[0]]
        return push(block, block, agb_s.at[s, n], agb_r.at[s, n], off)

    def gather_b(s):
        cps = [b_copy(s, n, (t, c, w), off) for n, off in enumerate(SAME_CORE + [PARTNER])]
        for cp in cps:
            cp.start()
        return cps

    def gram_part(s, k):
        bmat = jnp.concatenate([bcols[s, 2 * n + k].reshape(2 * rank, rank) for n in range(2)], axis=0)
        return dot_t0(bmat, bmat)

    def relay_b(s, cps):
        fwd = []
        for n, off in reversed(list(enumerate(SAME_CORE))):
            cps[n].wait()
            fwd.append(b_copy(s, 4 + n, dev(off), PARTNER))
            fwd[-1].start()
        cps[3].wait()
        gbp[...] = gram_part(s, core)
        for cp in fwd:
            cp.wait()
        gbp[...] += gram_part(s, 1 - core)
        for h in range(2):
            gram_copy(s, h).start()

    mid = rank // 2

    def gram_copy(s, h):
        part = pl.ds(h * mid, mid)
        return push(gbp.at[part], gbr.at[s, part], gb_s.at[s, h], gb_r.at[s, h], (0, 1, 0, 0))

    def gather_and_u(s, cps):
        relay_b(s, cps)

        def body(k, _):
            acc = None
            for n in range(4):
                p = jnp.dot(xh[k, n], bcols[s, n].reshape(2 * rank, rank), preferred_element_type=F32)
                acc = p if acc is None else acc + p
            u_ref[k] = acc
            return 0

        lax.fori_loop(0, kk, body, 0, unroll=8)

    def finish_gram_b(s, h):
        part = pl.ds(h * mid, mid)
        gram_copy(s, h).wait()
        gb_ref[part, :] = gbp[part, :] + gbr[s, part, :]

    def factor(gram_one, gram_two, ready=lambda h: None):
        rows = lax.broadcasted_iota(jnp.int32, (rank, rank), 0)
        cols = lax.broadcasted_iota(jnp.int32, (rank, rank), 1)
        eye = jnp.where(rows == cols, 1.0, 0.0).astype(F32)

        def fill(h):
            ready(h)
            part = slice(h * mid, (h + 1) * mid)
            w_ref[part, :rank] = gram_one[part, :] * gram_two[part, :] + lam_ref[0, 0] * eye[part, :]
            w_ref[part, rank:] = eye[part, :]

        r1 = lax.broadcasted_iota(jnp.int32, (8, rank), 0)

        def lane(x, n):
            return jnp.take_along_axis(x, jnp.full((8, rank), n, jnp.int32), axis=1, mode="promise_in_bounds")

        def spread(x, n):
            return jnp.broadcast_to(x[n : n + 1], (8, rank))

        def step(b, first, last):
            lo = pl.multiple_of(b * 8, 8)
            ps = w_ref[pl.ds(lo, 8), :rank]
            pi = w_ref[pl.ds(lo, 8), rank:]
            e = [lane(ps, lo + n) for n in range(8)]
            for n in range(8):
                for v in range(first, last):
                    e_ref[v, n] = lane(w_ref[8 * v : 8 * v + 8, :rank], lo + n)
            low_s = low_i = None
            piv = spread(e[0], 0)
            for j in range(8):
                isq = lax.rsqrt(piv)
                rc = isq * isq
                if j < 7:
                    x = spread(e[j + 1], j)
                    piv = spread(e[j + 1], j + 1) - (x * x) * rc
                m = e[j] * rc
                hit = r1 == j
                pjs = spread(ps, j)
                pji = spread(pi, j)
                low_s = pjs * isq if low_s is None else jnp.where(hit, pjs * isq, low_s)
                low_i = pji * isq if low_i is None else jnp.where(hit, pji * isq, low_i)
                ps = jnp.where(hit, pjs * rc, ps - m * pjs)
                pi = jnp.where(hit, pji * rc, pi - m * pji)
                for n in range(j + 1, 8):
                    en = spread(e[n], j)
                    e[n] = jnp.where(hit, en * rc, e[n] - m * en)
            li_ref[pl.ds(lo, 8), :rank] = low_s
            li_ref[pl.ds(lo, 8), rank:] = low_i
            qs = [spread(ps, n) for n in range(8)]
            qi = [spread(pi, n) for n in range(8)]
            for v in range(first, last):
                ds = [e_ref[v, n] * qs[n] for n in range(8)]
                di = [e_ref[v, n] * qi[n] for n in range(8)]
                while len(ds) > 1:
                    ds = [ds[n] + ds[n + 1] for n in range(0, len(ds), 2)]
                    di = [di[n] + di[n + 1] for n in range(0, len(di), 2)]
                w_ref[8 * v : 8 * v + 8, :rank] -= ds[0]
                w_ref[8 * v : 8 * v + 8, rank:] -= di[0]

        def run(lo, hi, first, last):
            def body(b, _):
                step(b, first, last)
                return 0

            lax.fori_loop(lo, hi, body, 0)

        half, end = rank // 16, rank // 8
        fill(0)
        run(0, half // 2, 0, half)
        run(half // 2, half, half // 2, half)
        fill(1)
        w_ref[mid:, :] = w_ref[mid:, :] - dot_t0(li_ref[:mid, mid:rank], li_ref[:mid, :], precision=HI)
        run(half, half + half // 2, half, end)
        run(half + half // 2, end, half + half // 2, end)

    cps = gather_b(0)

    lax.fori_loop(first, kk, load, 0)
    gather_and_u(0, cps)

    def sweep(s, _):
        c16 = cfac[...].astype(BF16)
        gram_c = dot_t0(c16, c16)

        def body_a(k, acc):
            return acc + u_ref[k] * cfac[pl.ds(t * kk + k, 1), :]

        part = lax.fori_loop(0, kk, body_a, jnp.zeros((ii, rank), F32))
        pa[...] = part.reshape(pa.shape)
        ra = []
        for n, off in enumerate(YZ):
            g2 = dev(off)[1] * 2 + dev(off)[0]
            ra.append(push(pa.at[g2], rsa.at[s, n], rsa_s.at[s, n], rsa_r.at[s, n], off))
        for cp in ra:
            cp.start()

        def ready_first(h):
            @pl.when(s == 0)
            def _():
                finish_gram_b(0, h)

        factor(gb_ref, gram_c, ready_first)
        inv_ref[...] = dot_t0(li_ref[:, rank:], li_ref[:, rank:], precision=HI)
        for cp in ra:
            cp.wait()
        mtt_a = pa[g] + rsa[s, 0] + rsa[s, 1] + rsa[s, 2]
        a_own = jnp.dot(mtt_a, inv_ref[...], precision=HI, preferred_element_type=F32)
        a16[s, w, g] = a_own.astype(BF16)
        af[s, g] = a_own
        ga = [
            push(a16.at[s, w, g], a16.at[s, w, g], aga_s.at[s, n], aga_r.at[s, n], off) for n, off in enumerate(YZ + YZ_FAR)
        ]
        for cp in ga:
            cp.start()
        out[: a_own.shape[0], :] = a_own

        cmine = cfac[pl.ds(pl.multiple_of(t * kk, kk), kk), :]
        ct = jnp.transpose(jnp.concatenate([cmine, jnp.zeros((rank - kk, rank), F32)], axis=0))
        for k in range(kk):
            cb[k] = jnp.broadcast_to(ct[:, k : k + 1], (rank, rank))
        for cp in ga[:3]:
            cp.wait()

        def hand_on(w2, n):
            return push(a16.at[s, w2], a16.at[s, w2], aga_s.at[s, n], aga_r.at[s, n], PARTNER)

        near = hand_on(w, 7)
        near.start()
        at_ref[...] = jnp.transpose(a16[s, w].reshape(ii, rank))

        def chunk(wc):
            def body(k, acc):
                ck = cb[k]
                return acc + jnp.dot(at_ref[...], xh[k, wc], preferred_element_type=F32) * jnp.concatenate([ck, ck], axis=1)

            return lax.fori_loop(0, kk, body, jnp.zeros((rank, ii), F32), unroll=16)

        vc = []
        for n in range(2):
            vp[n] = chunk(((xc + 1 - n) % 2) * 2 + (1 - core))
            vc.append(push(vp.at[n], vpr.at[s, n], vp_s.at[s, n], vp_r.at[s, n], (0, 0, 0, 1)))
            vc[n].start()
        for cp in ga[3:]:
            cp.wait()
        far = hand_on((1 - xc) * 2 + core, 8)
        far.start()
        rb = []
        for n in range(2):
            mine = chunk(((xc + 1 - n) % 2) * 2 + core)
            vc[n].wait()
            mine = mine + vpr[s, n]
            vo[n, 0] = mine[:, :rank]
            vo[n, 1] = mine[:, rank:]
            for off in ((1, 0, 1, 0), (0, 0, 1, 0)) if n == 0 else ((1, 0, 0, 0),):
                m = len(rb)
                rb.append(push(vo.at[n, dev(off)[0]], rsb.at[s, m], rsb_s.at[s, m], rsb_r.at[s, m], off))
                rb[m].start()
        fa = [push(af.at[s, g], af.at[s, g], af_s.at[s, n], af_r.at[s, n], off) for n, off in enumerate(YZ)]
        for cp in fa:
            cp.start()
        near.wait()
        far.wait()
        aall = a16[s].reshape(4 * ii, rank)
        ga_ref[...] = dot_t0(aall, aall)
        factor(ga_ref, gram_c)
        inv_ref[...] = dot_t0(li_ref[:, rank:], li_ref[:, rank:], precision=HI)
        for cp in rb:
            cp.wait()
        mtt_b = vo[1, t] + rsb[s, 0] + rsb[s, 1] + rsb[s, 2]
        b_own = jnp.transpose(jnp.dot(inv_ref[...], mtt_b, precision=HI, preferred_element_type=F32))
        bcols[s + 1, w, t] = b_own.astype(BF16)
        gcs = gather_b(s + 1)
        out[ii // 4 : ii // 4 + rank, :] = b_own

        gather_and_u(s + 1, gcs)
        for cp in fa:
            cp.wait()
        afull = af[s].reshape(ii, rank)
        pc[s, me] = jnp.concatenate(
            [jnp.sum(u_ref[k] * afull, axis=0, keepdims=True) for k in range(kk)], axis=0
        )
        cs = [push(pc.at[s, me], pc.at[s, me], pc_s.at[s, n], pc_r.at[s, n], off) for n, off in enumerate(ALL)]
        for cp in cs:
            cp.start()
        factor(ga_ref, gb_ref, lambda h: finish_gram_b(s + 1, h))
        inv_ref[...] = dot_t0(li_ref[:, rank:], li_ref[:, rank:], precision=HI)
        for cp in cs:
            cp.wait()
        halves = []
        for t2 in range(2):
            tot = None
            for c2 in range(2):
                for w2 in range(4):
                    term = pc[s, (c2 * 2 + t2) * 4 + w2]
                    tot = term if tot is None else tot + term
            halves.append(tot)
        cfac[...] = jnp.dot(jnp.concatenate(halves, axis=0), inv_ref[...], precision=HI, preferred_element_type=F32)
        return 0

    lax.fori_loop(0, SWEEPS, sweep, 0)
    out[ii // 4 + rank :, :] = cfac[...]


def split(rows, packed):
    def copy(src, *dsts):
        at = 0
        for n, dst in zip(rows, dsts):
            dst[...] = src[at : at + n, :]
            at += n

    vmem = pl.BlockSpec(memory_space=pltpu.VMEM)
    return pl.pallas_call(
        copy,
        name="results",
        out_shape=tuple(jax.ShapeDtypeStruct((n, packed.shape[1]), packed.dtype) for n in rows),
        in_specs=[vmem],
        out_specs=(vmem,) * len(rows),
        compiler_params=pltpu.CompilerParams(vmem_limit_bytes=1024 * 1024),
    )(packed)


def solution(mesh):
    def local_sweeps(x_blk, b_own, c_full, ridge_lam):
        kk, ii, jj = x_blk.shape
        brows, rank = b_own.shape
        arows, crows = ii // 4, c_full.shape[0]
        dma = pltpu.SemaphoreType.DMA
        vmem = pl.BlockSpec(memory_space=pltpu.VMEM)
        hbm = pl.BlockSpec(memory_space=pl.ANY)

        def sems(*shape):
            return [dma(shape), dma(shape)]

        packed = pl.pallas_call(
            kernel,
            name="als",
            out_shape=jax.ShapeDtypeStruct((arows + brows + crows, rank), F32),
            in_specs=[hbm, hbm, hbm, pl.BlockSpec(memory_space=pltpu.SMEM)],
            out_specs=vmem,
            scratch_shapes=[
                pltpu.VMEM((kk, ii, jj), F32),
                pltpu.VMEM((kk, jj // ii, ii, ii), BF16),
                pltpu.VMEM((kk, ii, rank), F32),
                pltpu.VMEM((brows, rank), F32),
                pltpu.VMEM((SWEEPS + 1, 4, 2, brows, rank), BF16),
                pltpu.VMEM((SWEEPS, 4, 4, arows, rank), BF16),
                pltpu.VMEM((rank, ii), BF16),
                pltpu.VMEM((SWEEPS, 4, arows, rank), F32),
                pltpu.VMEM((4, arows, rank), F32),
                pltpu.VMEM((SWEEPS, 3, arows, rank), F32),
                pltpu.VMEM((2, rank, 2 * brows), F32),
                pltpu.VMEM((SWEEPS, 2, rank, 2 * brows), F32),
                pltpu.VMEM((2, 2, rank, brows), F32),
                pltpu.VMEM((SWEEPS, 3, rank, brows), F32),
                pltpu.VMEM((rank, rank), F32),
                pltpu.VMEM((SWEEPS + 1, rank, rank), F32),
                pltpu.VMEM((SWEEPS, 16, kk, rank), F32),
                pltpu.VMEM((kk, rank, rank), F32),
                pltpu.VMEM((rank, 2 * rank), F32),
                pltpu.VMEM((rank // 8, 8, 8, rank), F32),
                pltpu.VMEM((rank, 2 * rank), F32),
                pltpu.VMEM((rank, rank), F32),
                pltpu.VMEM((rank, rank), F32),
                pltpu.VMEM((rank, rank), F32),
                pltpu.VMEM(c_full.shape, F32),
                dma((kk,)), dma((2,)),
                *sems(SWEEPS, 3), *sems(SWEEPS, 9), *sems(SWEEPS, 3), *sems(SWEEPS, 2), *sems(SWEEPS, 3),
                *sems(SWEEPS + 1, 7), *sems(SWEEPS + 1, 2), *sems(SWEEPS, 15),
            ],
            compiler_params=pltpu.CompilerParams(
                collective_id=0, has_side_effects=True, vmem_limit_bytes=56 * 1024 * 1024
            ),
        )(x_blk, b_own, c_full, ridge_lam.reshape(1, 1))
        return split((arows, brows, crows), packed)

    return jax.shard_map(
        local_sweeps,
        mesh=mesh,
        in_specs=(P("tube", "row", "col"), P(("col", "row", "tube"), None), P(None, None), P()),
        out_specs=(P(("row", "col", "tube"), None), P(("col", "row", "tube"), None), P(None, None)),
        check_vma=False,
    )
```

```python
import jax
import jax.numpy as jnp
from jax import lax
from jax.experimental import pallas as pl
from jax.experimental.pallas import tpu as pltpu
from jax.sharding import PartitionSpec as P

SWEEPS = 2
HI = lax.Precision.HIGHEST
MESH = pl.DeviceIdType.MESH
F32 = jnp.float32
BF16 = jnp.bfloat16

YZ = [(1, 1, 0, 0), (0, 1, 0, 0), (1, 0, 0, 0)]
SAME_CORE = [(1, 0, 1, 0), (0, 0, 1, 0), (1, 0, 0, 0)]
YZ_FAR = [(1, 1, 1, 0), (0, 1, 1, 0), (1, 0, 1, 0), (0, 0, 1, 0)]
PARTNER = (0, 0, 0, 1)
ALL = YZ + [(t, c, x, k) for x, k in ((1, 1), (1, 0), (0, 1)) for c in (1, 0) for t in (1, 0)]


def dot_t0(a, b, **kw):
    return lax.dot_general(a, b, (((0,), (0,)), ((), ())), preferred_element_type=F32, **kw)


def kernel(
    x_hbm, b_hbm, c_hbm, lam_hbm,
    out,
    lam_ref, xf, xh, u_ref, b_in, bcols, a16, at_ref, af, pa, rsa, vp, vpr, vo, rsb, gbp, gbr, pc, cb,
    w_ref, e_ref, li_ref, inv_ref, ga_ref, gb_ref, cfac,
    x_sem, in_sem, rsa_s, rsa_r, aga_s, aga_r, af_s, af_r, vp_s, vp_r, rsb_s, rsb_r, agb_s, agb_r, gb_s, gb_r, pc_s, pc_r,
):
    t = lax.axis_index("tube")
    c = lax.axis_index("col")
    w = lax.axis_index("row")
    xc, core = w // 2, w % 2
    kk, ii, jj = xf.shape
    rank = b_in.shape[1]
    g = c * 2 + t
    me = g * 4 + w

    ins = [
        pltpu.make_async_copy(b_hbm, b_in, in_sem.at[0]),
        pltpu.make_async_copy(c_hbm, cfac, in_sem.at[1]),
        pltpu.make_async_copy(lam_hbm, lam_ref, in_sem.at[2]),
    ]
    for cp in ins:
        cp.start()
    depth = 4
    for k in range(depth):
        pltpu.make_async_copy(x_hbm.at[k], xf.at[k], x_sem.at[k]).start()

    def load(k, _):
        pltpu.make_async_copy(x_hbm.at[k], xf.at[k], x_sem.at[k]).wait()

        @pl.when(k + depth < kk)
        def _():
            pltpu.make_async_copy(x_hbm.at[k + depth], xf.at[k + depth], x_sem.at[k + depth]).start()

        for n in range(jj // ii):
            xh[k, n] = xf[k, :, n * ii : (n + 1) * ii].astype(BF16)
        return 0

    def dev(off):
        return ((t + off[0]) % 2, (c + off[1]) % 2, ((xc + off[2]) % 2) * 2 + (core + off[3]) % 2)

    barrier = pltpu.get_barrier_semaphore()
    for off in reversed(ALL):
        pl.semaphore_signal(barrier, inc=1, device_id=dev(off), device_id_type=MESH)
    ins[0].wait()
    bcols[0, w, t] = b_in[...].astype(BF16)
    first = 4
    lax.fori_loop(0, first, load, 0)
    pl.semaphore_wait(barrier, len(ALL))

    def push(src, dst, ss, rs, off):
        return pltpu.make_async_remote_copy(
            src_ref=src, dst_ref=dst, send_sem=ss, recv_sem=rs, device_id=dev(off), device_id_type=MESH
        )

    def b_copy(s, n, src, off):
        block = bcols.at[s, src[2], src[0]]
        return push(block, block, agb_s.at[s, n], agb_r.at[s, n], off)

    def gather_b(s):
        cps = [b_copy(s, n, (t, c, w), off) for n, off in enumerate(SAME_CORE + [PARTNER])]
        for cp in cps:
            cp.start()
        return cps

    def gram_part(s, k):
        bmat = jnp.concatenate([bcols[s, 2 * n + k].reshape(2 * rank, rank) for n in range(2)], axis=0)
        return dot_t0(bmat, bmat)

    def relay_b(s, cps):
        fwd = []
        for n, off in reversed(list(enumerate(SAME_CORE))):
            cps[n].wait()
            fwd.append(b_copy(s, 4 + n, dev(off), PARTNER))
            fwd[-1].start()
        cps[3].wait()
        gbp[...] = gram_part(s, core)
        for cp in fwd:
            cp.wait()
        gbp[...] += gram_part(s, 1 - core)
        for h in range(2):
            gram_copy(s, h).start()

    mid = rank // 2

    def gram_copy(s, h):
        part = pl.ds(h * mid, mid)
        return push(gbp.at[part], gbr.at[s, part], gb_s.at[s, h], gb_r.at[s, h], (0, 1, 0, 0))

    def gather_and_u(s, cps):
        relay_b(s, cps)

        def body(k, _):
            acc = None
            for n in range(4):
                p = jnp.dot(xh[k, n], bcols[s, n].reshape(2 * rank, rank), preferred_element_type=F32)
                acc = p if acc is None else acc + p
            u_ref[k] = acc
            return 0

        lax.fori_loop(0, kk, body, 0, unroll=8)

    def finish_gram_b(s, h):
        part = pl.ds(h * mid, mid)
        gram_copy(s, h).wait()
        gb_ref[part, :] = gbp[part, :] + gbr[s, part, :]

    def factor(gram_one, gram_two, ready=lambda h: None):
        rows = lax.broadcasted_iota(jnp.int32, (rank, rank), 0)
        cols = lax.broadcasted_iota(jnp.int32, (rank, rank), 1)
        eye = jnp.where(rows == cols, 1.0, 0.0).astype(F32)

        def fill(h):
            ready(h)
            part = slice(h * mid, (h + 1) * mid)
            w_ref[part, :rank] = gram_one[part, :] * gram_two[part, :] + lam_ref[0, 0] * eye[part, :]
            w_ref[part, rank:] = eye[part, :]

        r1 = lax.broadcasted_iota(jnp.int32, (8, rank), 0)

        def lane(x, n):
            return jnp.take_along_axis(x, jnp.full((8, rank), n, jnp.int32), axis=1, mode="promise_in_bounds")

        def spread(x, n):
            return jnp.broadcast_to(x[n : n + 1], (8, rank))

        def step(b, first, last):
            lo = pl.multiple_of(b * 8, 8)
            ps = w_ref[pl.ds(lo, 8), :rank]
            pi = w_ref[pl.ds(lo, 8), rank:]
            e = [lane(ps, lo + n) for n in range(8)]
            for n in range(8):
                for v in range(first, last):
                    e_ref[v, n] = lane(w_ref[8 * v : 8 * v + 8, :rank], lo + n)
            low_s = low_i = None
            piv = spread(e[0], 0)
            for j in range(8):
                isq = lax.rsqrt(piv)
                rc = isq * isq
                if j < 7:
                    x = spread(e[j + 1], j)
                    piv = spread(e[j + 1], j + 1) - (x * x) * rc
                m = e[j] * rc
                hit = r1 == j
                pjs = spread(ps, j)
                pji = spread(pi, j)
                low_s = pjs * isq if low_s is None else jnp.where(hit, pjs * isq, low_s)
                low_i = pji * isq if low_i is None else jnp.where(hit, pji * isq, low_i)
                ps = jnp.where(hit, pjs * rc, ps - m * pjs)
                pi = jnp.where(hit, pji * rc, pi - m * pji)
                for n in range(j + 1, 8):
                    en = spread(e[n], j)
                    e[n] = jnp.where(hit, en * rc, e[n] - m * en)
            li_ref[pl.ds(lo, 8), :rank] = low_s
            li_ref[pl.ds(lo, 8), rank:] = low_i
            qs = [spread(ps, n) for n in range(8)]
            qi = [spread(pi, n) for n in range(8)]
            for v in range(first, last):
                ds = [e_ref[v, n] * qs[n] for n in range(8)]
                di = [e_ref[v, n] * qi[n] for n in range(8)]
                while len(ds) > 1:
                    ds = [ds[n] + ds[n + 1] for n in range(0, len(ds), 2)]
                    di = [di[n] + di[n + 1] for n in range(0, len(di), 2)]
                w_ref[8 * v : 8 * v + 8, :rank] -= ds[0]
                w_ref[8 * v : 8 * v + 8, rank:] -= di[0]

        def run(lo, hi, first, last):
            def body(b, _):
                step(b, first, last)
                return 0

            lax.fori_loop(lo, hi, body, 0)

        half, end = rank // 16, rank // 8
        fill(0)
        run(0, half // 2, 0, half)
        run(half // 2, half, half // 2, half)
        fill(1)
        w_ref[mid:, :] = w_ref[mid:, :] - dot_t0(li_ref[:mid, mid:rank], li_ref[:mid, :], precision=HI)
        run(half, half + half // 2, half, end)
        run(half + half // 2, end, half + half // 2, end)

    cps = gather_b(0)

    lax.fori_loop(first, kk, load, 0)
    for cp in ins[1:]:
        cp.wait()
    gather_and_u(0, cps)

    def sweep(s, _):
        c16 = cfac[...].astype(BF16)
        gram_c = dot_t0(c16, c16)

        def body_a(k, acc):
            return acc + u_ref[k] * cfac[pl.ds(t * kk + k, 1), :]

        part = lax.fori_loop(0, kk, body_a, jnp.zeros((ii, rank), F32))
        pa[...] = part.reshape(pa.shape)
        ra = []
        for n, off in enumerate(YZ):
            g2 = dev(off)[1] * 2 + dev(off)[0]
            ra.append(push(pa.at[g2], rsa.at[s, n], rsa_s.at[s, n], rsa_r.at[s, n], off))
        for cp in ra:
            cp.start()

        def ready_first(h):
            @pl.when(s == 0)
            def _():
                finish_gram_b(0, h)

        factor(gb_ref, gram_c, ready_first)
        inv_ref[...] = dot_t0(li_ref[:, rank:], li_ref[:, rank:], precision=HI)
        for cp in ra:
            cp.wait()
        mtt_a = pa[g] + rsa[s, 0] + rsa[s, 1] + rsa[s, 2]
        a_own = jnp.dot(mtt_a, inv_ref[...], precision=HI, preferred_element_type=F32)
        a16[s, w, g] = a_own.astype(BF16)
        af[s, g] = a_own
        ga = [
            push(a16.at[s, w, g], a16.at[s, w, g], aga_s.at[s, n], aga_r.at[s, n], off) for n, off in enumerate(YZ + YZ_FAR)
        ]
        for cp in ga:
            cp.start()
        out[: a_own.shape[0], :] = a_own

        cmine = cfac[pl.ds(pl.multiple_of(t * kk, kk), kk), :]
        ct = jnp.transpose(jnp.concatenate([cmine, jnp.zeros((rank - kk, rank), F32)], axis=0))
        for k in range(kk):
            cb[k] = jnp.broadcast_to(ct[:, k : k + 1], (rank, rank))
        for cp in ga[:3]:
            cp.wait()

        def hand_on(w2, n):
            return push(a16.at[s, w2], a16.at[s, w2], aga_s.at[s, n], aga_r.at[s, n], PARTNER)

        near = hand_on(w, 7)
        near.start()
        at_ref[...] = jnp.transpose(a16[s, w].reshape(ii, rank))

        def chunk(wc):
            def body(k, acc):
                ck = cb[k]
                return acc + jnp.dot(at_ref[...], xh[k, wc], preferred_element_type=F32) * jnp.concatenate([ck, ck], axis=1)

            return lax.fori_loop(0, kk, body, jnp.zeros((rank, ii), F32), unroll=16)

        vc = []
        for n in range(2):
            vp[n] = chunk(((xc + 1 - n) % 2) * 2 + (1 - core))
            vc.append(push(vp.at[n], vpr.at[s, n], vp_s.at[s, n], vp_r.at[s, n], (0, 0, 0, 1)))
            vc[n].start()
        for cp in ga[3:]:
            cp.wait()
        far = hand_on((1 - xc) * 2 + core, 8)
        far.start()
        rb = []
        for n in range(2):
            mine = chunk(((xc + 1 - n) % 2) * 2 + core)
            vc[n].wait()
            mine = mine + vpr[s, n]
            vo[n, 0] = mine[:, :rank]
            vo[n, 1] = mine[:, rank:]
            for off in ((1, 0, 1, 0), (0, 0, 1, 0)) if n == 0 else ((1, 0, 0, 0),):
                m = len(rb)
                rb.append(push(vo.at[n, dev(off)[0]], rsb.at[s, m], rsb_s.at[s, m], rsb_r.at[s, m], off))
                rb[m].start()
        fa = [push(af.at[s, g], af.at[s, g], af_s.at[s, n], af_r.at[s, n], off) for n, off in enumerate(YZ)]
        for cp in fa:
            cp.start()
        near.wait()
        far.wait()
        aall = a16[s].reshape(4 * ii, rank)
        ga_ref[...] = dot_t0(aall, aall)
        factor(ga_ref, gram_c)
        inv_ref[...] = dot_t0(li_ref[:, rank:], li_ref[:, rank:], precision=HI)
        for cp in rb:
            cp.wait()
        mtt_b = vo[1, t] + rsb[s, 0] + rsb[s, 1] + rsb[s, 2]
        b_own = jnp.transpose(jnp.dot(inv_ref[...], mtt_b, precision=HI, preferred_element_type=F32))
        bcols[s + 1, w, t] = b_own.astype(BF16)
        gcs = gather_b(s + 1)
        out[ii // 4 : ii // 4 + rank, :] = b_own

        gather_and_u(s + 1, gcs)
        for cp in fa:
            cp.wait()
        afull = af[s].reshape(ii, rank)
        pc[s, me] = jnp.concatenate(
            [jnp.sum(u_ref[k] * afull, axis=0, keepdims=True) for k in range(kk)], axis=0
        )
        cs = [push(pc.at[s, me], pc.at[s, me], pc_s.at[s, n], pc_r.at[s, n], off) for n, off in enumerate(ALL)]
        for cp in cs:
            cp.start()
        factor(ga_ref, gb_ref, lambda h: finish_gram_b(s + 1, h))
        inv_ref[...] = dot_t0(li_ref[:, rank:], li_ref[:, rank:], precision=HI)
        for cp in cs:
            cp.wait()
        halves = []
        for t2 in range(2):
            tot = None
            for c2 in range(2):
                for w2 in range(4):
                    term = pc[s, (c2 * 2 + t2) * 4 + w2]
                    tot = term if tot is None else tot + term
            halves.append(tot)
        cfac[...] = jnp.dot(jnp.concatenate(halves, axis=0), inv_ref[...], precision=HI, preferred_element_type=F32)
        return 0

    lax.fori_loop(0, SWEEPS, sweep, 0)
    out[ii // 4 + rank :, :] = cfac[...]


def split(rows, packed):
    def copy(src, *dsts):
        at = 0
        for n, dst in zip(rows, dsts):
            dst[...] = src[at : at + n, :]
            at += n

    vmem = pl.BlockSpec(memory_space=pltpu.VMEM)
    return pl.pallas_call(
        copy,
        name="results",
        out_shape=tuple(jax.ShapeDtypeStruct((n, packed.shape[1]), packed.dtype) for n in rows),
        in_specs=[vmem],
        out_specs=(vmem,) * len(rows),
        compiler_params=pltpu.CompilerParams(vmem_limit_bytes=1024 * 1024),
    )(packed)


def solution(mesh):
    def local_sweeps(x_blk, b_own, c_full, ridge_lam):
        kk, ii, jj = x_blk.shape
        brows, rank = b_own.shape
        arows, crows = ii // 4, c_full.shape[0]
        dma = pltpu.SemaphoreType.DMA
        vmem = pl.BlockSpec(memory_space=pltpu.VMEM)
        hbm = pl.BlockSpec(memory_space=pl.ANY)

        def sems(*shape):
            return [dma(shape), dma(shape)]

        packed = pl.pallas_call(
            kernel,
            name="als",
            out_shape=pltpu.VMEM((arows + brows + crows, rank), F32),
            in_specs=[hbm] * 4,
            out_specs=vmem,
            scratch_shapes=[
                pltpu.SMEM((1, 1), F32),
                pltpu.VMEM((kk, ii, jj), F32),
                pltpu.VMEM((kk, jj // ii, ii, ii), BF16),
                pltpu.VMEM((kk, ii, rank), F32),
                pltpu.VMEM((brows, rank), F32),
                pltpu.VMEM((SWEEPS + 1, 4, 2, brows, rank), BF16),
                pltpu.VMEM((SWEEPS, 4, 4, arows, rank), BF16),
                pltpu.VMEM((rank, ii), BF16),
                pltpu.VMEM((SWEEPS, 4, arows, rank), F32),
                pltpu.VMEM((4, arows, rank), F32),
                pltpu.VMEM((SWEEPS, 3, arows, rank), F32),
                pltpu.VMEM((2, rank, 2 * brows), F32),
                pltpu.VMEM((SWEEPS, 2, rank, 2 * brows), F32),
                pltpu.VMEM((2, 2, rank, brows), F32),
                pltpu.VMEM((SWEEPS, 3, rank, brows), F32),
                pltpu.VMEM((rank, rank), F32),
                pltpu.VMEM((SWEEPS + 1, rank, rank), F32),
                pltpu.VMEM((SWEEPS, 16, kk, rank), F32),
                pltpu.VMEM((kk, rank, rank), F32),
                pltpu.VMEM((rank, 2 * rank), F32),
                pltpu.VMEM((rank // 8, 8, 8, rank), F32),
                pltpu.VMEM((rank, 2 * rank), F32),
                pltpu.VMEM((rank, rank), F32),
                pltpu.VMEM((rank, rank), F32),
                pltpu.VMEM((rank, rank), F32),
                pltpu.VMEM(c_full.shape, F32),
                dma((kk,)), dma((3,)),
                *sems(SWEEPS, 3), *sems(SWEEPS, 9), *sems(SWEEPS, 3), *sems(SWEEPS, 2), *sems(SWEEPS, 3),
                *sems(SWEEPS + 1, 7), *sems(SWEEPS + 1, 2), *sems(SWEEPS, 15),
            ],
            compiler_params=pltpu.CompilerParams(
                collective_id=0, has_side_effects=True, vmem_limit_bytes=56 * 1024 * 1024
            ),
        )(x_blk, b_own, c_full, ridge_lam.reshape(1, 1))
        return split((arows, brows, crows), packed)

    return jax.shard_map(
        local_sweeps,
        mesh=mesh,
        in_specs=(P("tube", "row", "col"), P(("col", "row", "tube"), None), P(None, None), P()),
        out_specs=(P(("row", "col", "tube"), None), P(("col", "row", "tube"), None), P(None, None)),
        check_vma=False,
    )
```

```python
import jax
import jax.numpy as jnp
from jax import lax
from jax.experimental import pallas as pl
from jax.experimental.pallas import tpu as pltpu
from jax.sharding import PartitionSpec as P

SWEEPS = 2
HI = lax.Precision.HIGHEST
MESH = pl.DeviceIdType.MESH
F32 = jnp.float32
BF16 = jnp.bfloat16

YZ = [(1, 1, 0, 0), (0, 1, 0, 0), (1, 0, 0, 0)]
SAME_CORE = [(1, 0, 1, 0), (0, 0, 1, 0), (1, 0, 0, 0)]
YZ_FAR = [(1, 1, 1, 0), (0, 1, 1, 0), (1, 0, 1, 0), (0, 0, 1, 0)]
PARTNER = (0, 0, 0, 1)
ALL = YZ + [(t, c, x, k) for x, k in ((1, 1), (1, 0), (0, 1)) for c in (1, 0) for t in (1, 0)]


def dot_t0(a, b, **kw):
    return lax.dot_general(a, b, (((0,), (0,)), ((), ())), preferred_element_type=F32, **kw)


def kernel(
    x_hbm, b_hbm, c_hbm, lam_hbm,
    out,
    lam_ref, xf, xh, u_ref, b_in, bcols, a16, at_ref, af, pa, rsa, vp, vpr, vo, rsb, gbp, gbr, pc, cb,
    w_ref, e_ref, li_ref, inv_ref, ga_ref, gb_ref, cfac,
    x_sem, in_sem, rsa_s, rsa_r, aga_s, aga_r, af_s, af_r, vp_s, vp_r, rsb_s, rsb_r, agb_s, agb_r, gb_s, gb_r, pc_s, pc_r,
):
    t = lax.axis_index("tube")
    c = lax.axis_index("col")
    w = lax.axis_index("row")
    xc, core = w // 2, w % 2
    kk, ii, jj = xf.shape
    rank = b_in.shape[1]
    g = c * 2 + t
    me = g * 4 + w

    ins = [
        pltpu.make_async_copy(b_hbm, b_in, in_sem.at[0]),
        pltpu.make_async_copy(c_hbm, cfac, in_sem.at[1]),
        pltpu.make_async_copy(lam_hbm, lam_ref, in_sem.at[2]),
    ]
    for cp in ins:
        cp.start()
    depth = 4
    for k in range(depth):
        pltpu.make_async_copy(x_hbm.at[k], xf.at[k], x_sem.at[k]).start()

    def load(k, _):
        pltpu.make_async_copy(x_hbm.at[k], xf.at[k], x_sem.at[k]).wait()

        @pl.when(k + depth < kk)
        def _():
            pltpu.make_async_copy(x_hbm.at[k + depth], xf.at[k + depth], x_sem.at[k + depth]).start()

        for n in range(jj // ii):
            xh[k, n] = xf[k, :, n * ii : (n + 1) * ii].astype(BF16)
        return 0

    def dev(off):
        return ((t + off[0]) % 2, (c + off[1]) % 2, ((xc + off[2]) % 2) * 2 + (core + off[3]) % 2)

    barrier = pltpu.get_barrier_semaphore()
    for off in reversed(ALL):
        pl.semaphore_signal(barrier, inc=1, device_id=dev(off), device_id_type=MESH)
    ins[0].wait()
    bcols[0, w, t] = b_in[...].astype(BF16)
    first = 4
    lax.fori_loop(0, first, load, 0)
    pl.semaphore_wait(barrier, len(ALL))

    def push(src, dst, ss, rs, off):
        return pltpu.make_async_remote_copy(
            src_ref=src, dst_ref=dst, send_sem=ss, recv_sem=rs, device_id=dev(off), device_id_type=MESH
        )

    def b_copy(s, n, src, off):
        block = bcols.at[s, src[2], src[0]]
        return push(block, block, agb_s.at[s, n], agb_r.at[s, n], off)

    def gather_b(s):
        cps = [b_copy(s, n, (t, c, w), off) for n, off in enumerate(SAME_CORE + [PARTNER])]
        for cp in cps:
            cp.start()
        return cps

    def gram_part(s, k):
        bmat = jnp.concatenate([bcols[s, 2 * n + k].reshape(2 * rank, rank) for n in range(2)], axis=0)
        return dot_t0(bmat, bmat)

    def relay_b(s, cps):
        fwd = []
        for n, off in reversed(list(enumerate(SAME_CORE))):
            cps[n].wait()
            fwd.append(b_copy(s, 4 + n, dev(off), PARTNER))
            fwd[-1].start()
        cps[3].wait()
        gbp[...] = gram_part(s, core)
        for cp in fwd:
            cp.wait()
        gbp[...] += gram_part(s, 1 - core)
        for h in range(2):
            gram_copy(s, h).start()

    mid = rank // 2

    def gram_copy(s, h):
        part = pl.ds(h * mid, mid)
        return push(gbp.at[part], gbr.at[s, part], gb_s.at[s, h], gb_r.at[s, h], (0, 1, 0, 0))

    def gather_and_u(s, cps, each=lambda k, u: None):
        relay_b(s, cps)

        def body(k, _):
            acc = None
            for n in range(4):
                p = jnp.dot(xh[k, n], bcols[s, n].reshape(2 * rank, rank), preferred_element_type=F32)
                acc = p if acc is None else acc + p
            u_ref[k] = acc
            each(k, acc)
            return 0

        lax.fori_loop(0, kk, body, 0, unroll=8)

    def finish_gram_b(s, h):
        part = pl.ds(h * mid, mid)
        gram_copy(s, h).wait()
        gb_ref[part, :] = gbp[part, :] + gbr[s, part, :]

    def factor(gram_one, gram_two, ready=lambda h: None):
        rows = lax.broadcasted_iota(jnp.int32, (rank, rank), 0)
        cols = lax.broadcasted_iota(jnp.int32, (rank, rank), 1)
        eye = jnp.where(rows == cols, 1.0, 0.0).astype(F32)

        def fill(h):
            ready(h)
            part = slice(h * mid, (h + 1) * mid)
            w_ref[part, :rank] = gram_one[part, :] * gram_two[part, :] + lam_ref[0, 0] * eye[part, :]
            w_ref[part, rank:] = eye[part, :]

        r1 = lax.broadcasted_iota(jnp.int32, (8, rank), 0)

        def lane(x, n):
            return jnp.take_along_axis(x, jnp.full((8, rank), n, jnp.int32), axis=1, mode="promise_in_bounds")

        def spread(x, n):
            return jnp.broadcast_to(x[n : n + 1], (8, rank))

        def step(b, first, last):
            lo = pl.multiple_of(b * 8, 8)
            ps = w_ref[pl.ds(lo, 8), :rank]
            pi = w_ref[pl.ds(lo, 8), rank:]
            e = [lane(ps, lo + n) for n in range(8)]
            for n in range(8):
                for v in range(first, last):
                    e_ref[v, n] = lane(w_ref[8 * v : 8 * v + 8, :rank], lo + n)
            low_s = low_i = None
            piv = spread(e[0], 0)
            for j in range(8):
                isq = lax.rsqrt(piv)
                rc = isq * isq
                if j < 7:
                    x = spread(e[j + 1], j)
                    piv = spread(e[j + 1], j + 1) - (x * x) * rc
                m = e[j] * rc
                hit = r1 == j
                pjs = spread(ps, j)
                pji = spread(pi, j)
                low_s = pjs * isq if low_s is None else jnp.where(hit, pjs * isq, low_s)
                low_i = pji * isq if low_i is None else jnp.where(hit, pji * isq, low_i)
                ps = jnp.where(hit, pjs * rc, ps - m * pjs)
                pi = jnp.where(hit, pji * rc, pi - m * pji)
                for n in range(j + 1, 8):
                    en = spread(e[n], j)
                    e[n] = jnp.where(hit, en * rc, e[n] - m * en)
            li_ref[pl.ds(lo, 8), :rank] = low_s
            li_ref[pl.ds(lo, 8), rank:] = low_i
            qs = [spread(ps, n) for n in range(8)]
            qi = [spread(pi, n) for n in range(8)]
            for v in range(first, last):
                ds = [e_ref[v, n] * qs[n] for n in range(8)]
                di = [e_ref[v, n] * qi[n] for n in range(8)]
                while len(ds) > 1:
                    ds = [ds[n] + ds[n + 1] for n in range(0, len(ds), 2)]
                    di = [di[n] + di[n + 1] for n in range(0, len(di), 2)]
                w_ref[8 * v : 8 * v + 8, :rank] -= ds[0]
                w_ref[8 * v : 8 * v + 8, rank:] -= di[0]

        def run(lo, hi, first, last):
            def body(b, _):
                step(b, first, last)
                return 0

            lax.fori_loop(lo, hi, body, 0)

        half, end = rank // 16, rank // 8
        fill(0)
        run(0, half // 2, 0, half)
        run(half // 2, half, half // 2, half)
        fill(1)
        w_ref[mid:, :] = w_ref[mid:, :] - dot_t0(li_ref[:mid, mid:rank], li_ref[:mid, :], precision=HI)
        run(half, half + half // 2, half, end)
        run(half + half // 2, end, half + half // 2, end)

    cps = gather_b(0)

    lax.fori_loop(first, kk, load, 0)
    for cp in ins[1:]:
        cp.wait()
    gather_and_u(0, cps)

    def sweep(s, _):
        c16 = cfac[...].astype(BF16)
        gram_c = dot_t0(c16, c16)

        def sum_rows(g2):
            part = pl.ds(pl.multiple_of(g2 * pa.shape[1], 8), pa.shape[1])

            def body(k, acc):
                return acc + u_ref[k, part, :] * cfac[pl.ds(t * kk + k, 1), :]

            pa[g2] = lax.fori_loop(0, kk, body, jnp.zeros(pa.shape[1:], F32), unroll=8)

        ra = []
        for n, off in enumerate(YZ):
            g2 = dev(off)[1] * 2 + dev(off)[0]
            sum_rows(g2)
            ra.append(push(pa.at[g2], rsa.at[s, n], rsa_s.at[s, n], rsa_r.at[s, n], off))
            ra[n].start()
        sum_rows(g)

        def ready_first(h):
            @pl.when(s == 0)
            def _():
                finish_gram_b(0, h)

        factor(gb_ref, gram_c, ready_first)
        inv_ref[...] = dot_t0(li_ref[:, rank:], li_ref[:, rank:], precision=HI)
        for cp in ra:
            cp.wait()
        mtt_a = pa[g] + rsa[s, 0] + rsa[s, 1] + rsa[s, 2]
        a_own = jnp.dot(mtt_a, inv_ref[...], precision=HI, preferred_element_type=F32)
        a16[s, w, g] = a_own.astype(BF16)
        af[s, g] = a_own
        ga = [
            push(a16.at[s, w, g], a16.at[s, w, g], aga_s.at[s, n], aga_r.at[s, n], off) for n, off in enumerate(YZ + YZ_FAR)
        ]
        for cp in ga:
            cp.start()
        out[: a_own.shape[0], :] = a_own

        cmine = cfac[pl.ds(pl.multiple_of(t * kk, kk), kk), :]
        ct = jnp.transpose(jnp.concatenate([cmine, jnp.zeros((rank - kk, rank), F32)], axis=0))
        for k in range(kk):
            cb[k] = jnp.broadcast_to(ct[:, k : k + 1], (rank, rank))
        for cp in ga[:3]:
            cp.wait()

        def hand_on(w2, n):
            return push(a16.at[s, w2], a16.at[s, w2], aga_s.at[s, n], aga_r.at[s, n], PARTNER)

        near = hand_on(w, 7)
        near.start()
        at_ref[...] = jnp.transpose(a16[s, w].reshape(ii, rank))

        def chunk(wc):
            def body(k, acc):
                ck = cb[k]
                return acc + jnp.dot(at_ref[...], xh[k, wc], preferred_element_type=F32) * jnp.concatenate([ck, ck], axis=1)

            return lax.fori_loop(0, kk, body, jnp.zeros((rank, ii), F32), unroll=16)

        vc = []
        for n in range(2):
            vp[n] = chunk(((xc + 1 - n) % 2) * 2 + (1 - core))
            vc.append(push(vp.at[n], vpr.at[s, n], vp_s.at[s, n], vp_r.at[s, n], (0, 0, 0, 1)))
            vc[n].start()
        for cp in ga[3:]:
            cp.wait()
        far = hand_on((1 - xc) * 2 + core, 8)
        far.start()
        rb = []
        for n in range(2):
            mine = chunk(((xc + 1 - n) % 2) * 2 + core)
            vc[n].wait()
            mine = mine + vpr[s, n]
            vo[n, 0] = mine[:, :rank]
            vo[n, 1] = mine[:, rank:]
            for off in ((1, 0, 1, 0), (0, 0, 1, 0)) if n == 0 else ((1, 0, 0, 0),):
                m = len(rb)
                rb.append(push(vo.at[n, dev(off)[0]], rsb.at[s, m], rsb_s.at[s, m], rsb_r.at[s, m], off))
                rb[m].start()
        fa = [push(af.at[s, g], af.at[s, g], af_s.at[s, n], af_r.at[s, n], off) for n, off in enumerate(YZ)]
        for cp in fa:
            cp.start()
        near.wait()
        far.wait()
        aall = a16[s].reshape(4 * ii, rank)
        ga_ref[...] = dot_t0(aall, aall)
        factor(ga_ref, gram_c)
        inv_ref[...] = dot_t0(li_ref[:, rank:], li_ref[:, rank:], precision=HI)
        for cp in rb:
            cp.wait()
        mtt_b = vo[1, t] + rsb[s, 0] + rsb[s, 1] + rsb[s, 2]
        b_own = jnp.transpose(jnp.dot(inv_ref[...], mtt_b, precision=HI, preferred_element_type=F32))
        bcols[s + 1, w, t] = b_own.astype(BF16)
        gcs = gather_b(s + 1)
        out[ii // 4 : ii // 4 + rank, :] = b_own

        for cp in fa:
            cp.wait()

        def part_c(k, u):
            pc[s, me, pl.ds(k, 1), :] = jnp.sum(u * af[s].reshape(ii, rank), axis=0, keepdims=True)

        gather_and_u(s + 1, gcs, part_c)
        cs = [push(pc.at[s, me], pc.at[s, me], pc_s.at[s, n], pc_r.at[s, n], off) for n, off in enumerate(ALL)]
        for cp in cs:
            cp.start()
        factor(ga_ref, gb_ref, lambda h: finish_gram_b(s + 1, h))
        inv_ref[...] = dot_t0(li_ref[:, rank:], li_ref[:, rank:], precision=HI)
        for cp in cs:
            cp.wait()
        halves = []
        for t2 in range(2):
            tot = None
            for c2 in range(2):
                for w2 in range(4):
                    term = pc[s, (c2 * 2 + t2) * 4 + w2]
                    tot = term if tot is None else tot + term
            halves.append(tot)
        cfac[...] = jnp.dot(jnp.concatenate(halves, axis=0), inv_ref[...], precision=HI, preferred_element_type=F32)
        return 0

    lax.fori_loop(0, SWEEPS, sweep, 0)
    out[ii // 4 + rank :, :] = cfac[...]


def split(rows, packed):
    def copy(src, *dsts):
        at = 0
        for n, dst in zip(rows, dsts):
            dst[...] = src[at : at + n, :]
            at += n

    vmem = pl.BlockSpec(memory_space=pltpu.VMEM)
    return pl.pallas_call(
        copy,
        name="results",
        out_shape=tuple(jax.ShapeDtypeStruct((n, packed.shape[1]), packed.dtype) for n in rows),
        in_specs=[vmem],
        out_specs=(vmem,) * len(rows),
        compiler_params=pltpu.CompilerParams(vmem_limit_bytes=1024 * 1024),
    )(packed)


def solution(mesh):
    def local_sweeps(x_blk, b_own, c_full, ridge_lam):
        kk, ii, jj = x_blk.shape
        brows, rank = b_own.shape
        arows, crows = ii // 4, c_full.shape[0]
        dma = pltpu.SemaphoreType.DMA
        vmem = pl.BlockSpec(memory_space=pltpu.VMEM)
        hbm = pl.BlockSpec(memory_space=pl.ANY)

        def sems(*shape):
            return [dma(shape), dma(shape)]

        packed = pl.pallas_call(
            kernel,
            name="als",
            out_shape=pltpu.VMEM((arows + brows + crows, rank), F32),
            in_specs=[hbm] * 4,
            out_specs=vmem,
            scratch_shapes=[
                pltpu.SMEM((1, 1), F32),
                pltpu.VMEM((kk, ii, jj), F32),
                pltpu.VMEM((kk, jj // ii, ii, ii), BF16),
                pltpu.VMEM((kk, ii, rank), F32),
                pltpu.VMEM((brows, rank), F32),
                pltpu.VMEM((SWEEPS + 1, 4, 2, brows, rank), BF16),
                pltpu.VMEM((SWEEPS, 4, 4, arows, rank), BF16),
                pltpu.VMEM((rank, ii), BF16),
                pltpu.VMEM((SWEEPS, 4, arows, rank), F32),
                pltpu.VMEM((4, arows, rank), F32),
                pltpu.VMEM((SWEEPS, 3, arows, rank), F32),
                pltpu.VMEM((2, rank, 2 * brows), F32),
                pltpu.VMEM((SWEEPS, 2, rank, 2 * brows), F32),
                pltpu.VMEM((2, 2, rank, brows), F32),
                pltpu.VMEM((SWEEPS, 3, rank, brows), F32),
                pltpu.VMEM((rank, rank), F32),
                pltpu.VMEM((SWEEPS + 1, rank, rank), F32),
                pltpu.VMEM((SWEEPS, 16, kk, rank), F32),
                pltpu.VMEM((kk, rank, rank), F32),
                pltpu.VMEM((rank, 2 * rank), F32),
                pltpu.VMEM((rank // 8, 8, 8, rank), F32),
                pltpu.VMEM((rank, 2 * rank), F32),
                pltpu.VMEM((rank, rank), F32),
                pltpu.VMEM((rank, rank), F32),
                pltpu.VMEM((rank, rank), F32),
                pltpu.VMEM(c_full.shape, F32),
                dma((kk,)), dma((3,)),
                *sems(SWEEPS, 3), *sems(SWEEPS, 9), *sems(SWEEPS, 3), *sems(SWEEPS, 2), *sems(SWEEPS, 3),
                *sems(SWEEPS + 1, 7), *sems(SWEEPS + 1, 2), *sems(SWEEPS, 15),
            ],
            compiler_params=pltpu.CompilerParams(
                collective_id=0, has_side_effects=True, vmem_limit_bytes=56 * 1024 * 1024
            ),
        )(x_blk, b_own, c_full, ridge_lam.reshape(1, 1))
        return split((arows, brows, crows), packed)

    return jax.shard_map(
        local_sweeps,
        mesh=mesh,
        in_specs=(P("tube", "row", "col"), P(("col", "row", "tube"), None), P(None, None), P()),
        out_specs=(P(("row", "col", "tube"), None), P(("col", "row", "tube"), None), P(None, None)),
        check_vma=False,
    )
```

```python
import jax
import jax.numpy as jnp
from jax import lax
from jax.experimental import pallas as pl
from jax.experimental.pallas import tpu as pltpu
from jax.sharding import PartitionSpec as P

SWEEPS = 2
HI = lax.Precision.HIGHEST
MESH = pl.DeviceIdType.MESH
F32 = jnp.float32
BF16 = jnp.bfloat16

YZ = [(1, 1, 0, 0), (0, 1, 0, 0), (1, 0, 0, 0)]
SAME_CORE = [(1, 0, 1, 0), (0, 0, 1, 0), (1, 0, 0, 0)]
YZ_FAR = [(1, 1, 1, 0), (0, 1, 1, 0), (1, 0, 1, 0), (0, 0, 1, 0)]
PARTNER = (0, 0, 0, 1)
ALL = YZ + [(t, c, x, k) for x, k in ((1, 1), (1, 0), (0, 1)) for c in (1, 0) for t in (1, 0)]


def dot_t0(a, b, **kw):
    return lax.dot_general(a, b, (((0,), (0,)), ((), ())), preferred_element_type=F32, **kw)


def kernel(
    x_hbm, b_hbm, c_hbm, lam_hbm,
    out,
    lam_ref, xf, xh, u_ref, b_in, bcols, a16, at_ref, af, pa, rsa, vp, vpr, vo, rsb, gbp, gbr, pc, cb,
    w_ref, e_ref, li_ref, inv_ref, ga_ref, gb_ref, cfac,
    x_sem, in_sem, rsa_s, rsa_r, aga_s, aga_r, af_s, af_r, vp_s, vp_r, rsb_s, rsb_r, agb_s, agb_r, gb_s, gb_r, pc_s, pc_r,
):
    t = lax.axis_index("tube")
    c = lax.axis_index("col")
    w = lax.axis_index("row")
    xc, core = w // 2, w % 2
    kk, ii, jj = xf.shape
    rank = b_in.shape[1]
    g = c * 2 + t
    me = g * 4 + w

    ins = [
        pltpu.make_async_copy(b_hbm, b_in, in_sem.at[0]),
        pltpu.make_async_copy(c_hbm, cfac, in_sem.at[1]),
        pltpu.make_async_copy(lam_hbm, lam_ref, in_sem.at[2]),
    ]
    for cp in ins:
        cp.start()
    depth = 5
    for k in range(depth):
        pltpu.make_async_copy(x_hbm.at[k], xf.at[k], x_sem.at[k]).start()

    def load(k, _):
        pltpu.make_async_copy(x_hbm.at[k], xf.at[k], x_sem.at[k]).wait()

        @pl.when(k + depth < kk)
        def _():
            pltpu.make_async_copy(x_hbm.at[k + depth], xf.at[k + depth], x_sem.at[k + depth]).start()

        for n in range(jj // ii):
            xh[k, n] = xf[k, :, n * ii : (n + 1) * ii].astype(BF16)
        return 0

    def dev(off):
        return ((t + off[0]) % 2, (c + off[1]) % 2, ((xc + off[2]) % 2) * 2 + (core + off[3]) % 2)

    barrier = pltpu.get_barrier_semaphore()
    for off in reversed(ALL):
        pl.semaphore_signal(barrier, inc=1, device_id=dev(off), device_id_type=MESH)
    ins[0].wait()
    bcols[0, w, t] = b_in[...].astype(BF16)
    first = 4
    lax.fori_loop(0, first, load, 0)
    pl.semaphore_wait(barrier, len(ALL))

    def push(src, dst, ss, rs, off):
        return pltpu.make_async_remote_copy(
            src_ref=src, dst_ref=dst, send_sem=ss, recv_sem=rs, device_id=dev(off), device_id_type=MESH
        )

    def b_copy(s, n, src, off):
        block = bcols.at[s, src[2], src[0]]
        return push(block, block, agb_s.at[s, n], agb_r.at[s, n], off)

    def gather_b(s):
        cps = [b_copy(s, n, (t, c, w), off) for n, off in enumerate(SAME_CORE + [PARTNER])]
        for cp in cps:
            cp.start()
        return cps

    def gram_part(s, k):
        bmat = jnp.concatenate([bcols[s, 2 * n + k].reshape(2 * rank, rank) for n in range(2)], axis=0)
        return dot_t0(bmat, bmat)

    def relay_b(s, cps):
        fwd = []
        for n, off in reversed(list(enumerate(SAME_CORE))):
            cps[n].wait()
            fwd.append(b_copy(s, 4 + n, dev(off), PARTNER))
            fwd[-1].start()
        cps[3].wait()
        gbp[...] = gram_part(s, core)
        for cp in fwd:
            cp.wait()
        gbp[...] += gram_part(s, 1 - core)
        for h in range(2):
            gram_copy(s, h).start()

    mid = rank // 2

    def gram_copy(s, h):
        part = pl.ds(h * mid, mid)
        return push(gbp.at[part], gbr.at[s, part], gb_s.at[s, h], gb_r.at[s, h], (0, 1, 0, 0))

    def gather_and_u(s, cps, each=lambda k, u: None):
        relay_b(s, cps)

        def body(k, _):
            acc = None
            for n in range(4):
                p = jnp.dot(xh[k, n], bcols[s, n].reshape(2 * rank, rank), preferred_element_type=F32)
                acc = p if acc is None else acc + p
            u_ref[k] = acc
            each(k, acc)
            return 0

        lax.fori_loop(0, kk, body, 0, unroll=8)

    def finish_gram_b(s, h):
        part = pl.ds(h * mid, mid)
        gram_copy(s, h).wait()
        gb_ref[part, :] = gbp[part, :] + gbr[s, part, :]

    def factor(gram_one, gram_two, ready=lambda h: None, by=4):
        rows = lax.broadcasted_iota(jnp.int32, (rank, rank), 0)
        cols = lax.broadcasted_iota(jnp.int32, (rank, rank), 1)
        eye = jnp.where(rows == cols, 1.0, 0.0).astype(F32)

        def fill(h):
            ready(h)
            part = slice(h * mid, (h + 1) * mid)
            w_ref[part, :rank] = gram_one[part, :] * gram_two[part, :] + lam_ref[0, 0] * eye[part, :]
            w_ref[part, rank:] = eye[part, :]

        r1 = lax.broadcasted_iota(jnp.int32, (8, rank), 0)

        def lane(x, n):
            return jnp.take_along_axis(x, jnp.full((8, rank), n, jnp.int32), axis=1, mode="promise_in_bounds")

        def spread(x, n):
            return jnp.broadcast_to(x[n : n + 1], (8, rank))

        def step(b, first, last):
            lo = pl.multiple_of(b * 8, 8)
            ps = w_ref[pl.ds(lo, 8), :rank]
            pi = w_ref[pl.ds(lo, 8), rank:]
            e = [lane(ps, lo + n) for n in range(8)]
            for n in range(8):
                for v in range(first, last):
                    e_ref[v, n] = lane(w_ref[8 * v : 8 * v + 8, :rank], lo + n)
            low_s = low_i = None
            piv = spread(e[0], 0)
            for j in range(8):
                isq = lax.rsqrt(piv)
                rc = isq * isq
                if j < 7:
                    x = spread(e[j + 1], j)
                    piv = spread(e[j + 1], j + 1) - (x * x) * rc
                m = e[j] * rc
                hit = r1 == j
                pjs = spread(ps, j)
                pji = spread(pi, j)
                low_s = pjs * isq if low_s is None else jnp.where(hit, pjs * isq, low_s)
                low_i = pji * isq if low_i is None else jnp.where(hit, pji * isq, low_i)
                ps = jnp.where(hit, pjs * rc, ps - m * pjs)
                pi = jnp.where(hit, pji * rc, pi - m * pji)
                for n in range(j + 1, 8):
                    en = spread(e[n], j)
                    e[n] = jnp.where(hit, en * rc, e[n] - m * en)
            li_ref[pl.ds(lo, 8), :rank] = low_s
            li_ref[pl.ds(lo, 8), rank:] = low_i
            qs = [spread(ps, n) for n in range(8)]
            qi = [spread(pi, n) for n in range(8)]
            for v in range(first, last):
                ds = [e_ref[v, n] * qs[n] for n in range(8)]
                di = [e_ref[v, n] * qi[n] for n in range(8)]
                while len(ds) > 1:
                    ds = [ds[n] + ds[n + 1] for n in range(0, len(ds), 2)]
                    di = [di[n] + di[n + 1] for n in range(0, len(di), 2)]
                w_ref[8 * v : 8 * v + 8, :rank] -= ds[0]
                w_ref[8 * v : 8 * v + 8, rank:] -= di[0]

        def run(lo, hi, first, last):
            def body(b, _):
                step(b, first, last)
                return 0

            lax.fori_loop(lo, hi, body, 0)

        half, end = rank // 16, rank // 8
        fill(0)
        for n in range(0, half, by):
            run(n, n + by, n, half)
        fill(1)
        w_ref[mid:, :] = w_ref[mid:, :] - dot_t0(li_ref[:mid, mid:rank], li_ref[:mid, :], precision=HI)
        for n in range(half, end, by):
            run(n, n + by, n, end)

    cps = gather_b(0)

    lax.fori_loop(first, kk, load, 0)
    for cp in ins[1:]:
        cp.wait()
    gather_and_u(0, cps)

    def sweep(s, _):
        c16 = cfac[...].astype(BF16)
        gram_c = dot_t0(c16, c16)

        def sum_rows(g2):
            part = pl.ds(pl.multiple_of(g2 * pa.shape[1], 8), pa.shape[1])

            def body(k, acc):
                return acc + u_ref[k, part, :] * cfac[pl.ds(t * kk + k, 1), :]

            pa[g2] = lax.fori_loop(0, kk, body, jnp.zeros(pa.shape[1:], F32), unroll=8)

        ra = []
        for n, off in enumerate(YZ):
            g2 = dev(off)[1] * 2 + dev(off)[0]
            sum_rows(g2)
            ra.append(push(pa.at[g2], rsa.at[s, n], rsa_s.at[s, n], rsa_r.at[s, n], off))
            ra[n].start()
        sum_rows(g)

        def ready_first(h):
            @pl.when(s == 0)
            def _():
                finish_gram_b(0, h)

        factor(gb_ref, gram_c, ready_first, by=2)
        inv_ref[...] = dot_t0(li_ref[:, rank:], li_ref[:, rank:], precision=HI)
        for cp in ra:
            cp.wait()
        mtt_a = pa[g] + rsa[s, 0] + rsa[s, 1] + rsa[s, 2]
        a_own = jnp.dot(mtt_a, inv_ref[...], precision=HI, preferred_element_type=F32)
        a16[s, w, g] = a_own.astype(BF16)
        af[s, g] = a_own
        ga = [
            push(a16.at[s, w, g], a16.at[s, w, g], aga_s.at[s, n], aga_r.at[s, n], off) for n, off in enumerate(YZ + YZ_FAR)
        ]
        for cp in ga:
            cp.start()
        out[: a_own.shape[0], :] = a_own

        cmine = cfac[pl.ds(pl.multiple_of(t * kk, kk), kk), :]
        ct = jnp.transpose(jnp.concatenate([cmine, jnp.zeros((rank - kk, rank), F32)], axis=0))
        for k in range(kk):
            cb[k] = jnp.broadcast_to(ct[:, k : k + 1], (rank, rank))
        for cp in ga[:3]:
            cp.wait()

        def hand_on(w2, n):
            return push(a16.at[s, w2], a16.at[s, w2], aga_s.at[s, n], aga_r.at[s, n], PARTNER)

        near = hand_on(w, 7)
        near.start()
        at_ref[...] = jnp.transpose(a16[s, w].reshape(ii, rank))

        def chunk(wc):
            def body(k, acc):
                ck = cb[k]
                return acc + jnp.dot(at_ref[...], xh[k, wc], preferred_element_type=F32) * jnp.concatenate([ck, ck], axis=1)

            return lax.fori_loop(0, kk, body, jnp.zeros((rank, ii), F32), unroll=16)

        vc = []
        for n in range(2):
            vp[n] = chunk(((xc + 1 - n) % 2) * 2 + (1 - core))
            vc.append(push(vp.at[n], vpr.at[s, n], vp_s.at[s, n], vp_r.at[s, n], (0, 0, 0, 1)))
            vc[n].start()
        for cp in ga[3:]:
            cp.wait()
        far = hand_on((1 - xc) * 2 + core, 8)
        far.start()
        rb = []
        for n in range(2):
            mine = chunk(((xc + 1 - n) % 2) * 2 + core)
            vc[n].wait()
            mine = mine + vpr[s, n]
            vo[n, 0] = mine[:, :rank]
            vo[n, 1] = mine[:, rank:]
            for off in ((1, 0, 1, 0), (0, 0, 1, 0)) if n == 0 else ((1, 0, 0, 0),):
                m = len(rb)
                rb.append(push(vo.at[n, dev(off)[0]], rsb.at[s, m], rsb_s.at[s, m], rsb_r.at[s, m], off))
                rb[m].start()
        fa = [push(af.at[s, g], af.at[s, g], af_s.at[s, n], af_r.at[s, n], off) for n, off in enumerate(YZ)]
        for cp in fa:
            cp.start()
        near.wait()
        far.wait()
        aall = a16[s].reshape(4 * ii, rank)
        ga_ref[...] = dot_t0(aall, aall)
        factor(ga_ref, gram_c)
        inv_ref[...] = dot_t0(li_ref[:, rank:], li_ref[:, rank:], precision=HI)
        for cp in rb:
            cp.wait()
        mtt_b = vo[1, t] + rsb[s, 0] + rsb[s, 1] + rsb[s, 2]
        b_own = jnp.transpose(jnp.dot(inv_ref[...], mtt_b, precision=HI, preferred_element_type=F32))
        bcols[s + 1, w, t] = b_own.astype(BF16)
        gcs = gather_b(s + 1)
        out[ii // 4 : ii // 4 + rank, :] = b_own

        for cp in fa:
            cp.wait()

        def part_c(k, u):
            pc[s, me, pl.ds(k, 1), :] = jnp.sum(u * af[s].reshape(ii, rank), axis=0, keepdims=True)

        gather_and_u(s + 1, gcs, part_c)
        cs = [push(pc.at[s, me], pc.at[s, me], pc_s.at[s, n], pc_r.at[s, n], off) for n, off in enumerate(ALL)]
        for cp in cs:
            cp.start()
        factor(ga_ref, gb_ref, lambda h: finish_gram_b(s + 1, h))
        inv_ref[...] = dot_t0(li_ref[:, rank:], li_ref[:, rank:], precision=HI)
        for cp in cs:
            cp.wait()
        halves = []
        for t2 in range(2):
            tot = None
            for c2 in range(2):
                for w2 in range(4):
                    term = pc[s, (c2 * 2 + t2) * 4 + w2]
                    tot = term if tot is None else tot + term
            halves.append(tot)
        cfac[...] = jnp.dot(jnp.concatenate(halves, axis=0), inv_ref[...], precision=HI, preferred_element_type=F32)
        return 0

    lax.fori_loop(0, SWEEPS, sweep, 0)
    out[ii // 4 + rank :, :] = cfac[...]


def split(rows, packed):
    def copy(src, *dsts):
        at = 0
        for n, dst in zip(rows, dsts):
            dst[...] = src[at : at + n, :]
            at += n

    vmem = pl.BlockSpec(memory_space=pltpu.VMEM)
    return pl.pallas_call(
        copy,
        name="results",
        out_shape=tuple(jax.ShapeDtypeStruct((n, packed.shape[1]), packed.dtype) for n in rows),
        in_specs=[vmem],
        out_specs=(vmem,) * len(rows),
        compiler_params=pltpu.CompilerParams(vmem_limit_bytes=1024 * 1024),
    )(packed)


def solution(mesh):
    def local_sweeps(x_blk, b_own, c_full, ridge_lam):
        kk, ii, jj = x_blk.shape
        brows, rank = b_own.shape
        arows, crows = ii // 4, c_full.shape[0]
        dma = pltpu.SemaphoreType.DMA
        vmem = pl.BlockSpec(memory_space=pltpu.VMEM)
        hbm = pl.BlockSpec(memory_space=pl.ANY)

        def sems(*shape):
            return [dma(shape), dma(shape)]

        packed = pl.pallas_call(
            kernel,
            name="als",
            out_shape=pltpu.VMEM((arows + brows + crows, rank), F32),
            in_specs=[hbm] * 4,
            out_specs=vmem,
            scratch_shapes=[
                pltpu.SMEM((1, 1), F32),
                pltpu.VMEM((kk, ii, jj), F32),
                pltpu.VMEM((kk, jj // ii, ii, ii), BF16),
                pltpu.VMEM((kk, ii, rank), F32),
                pltpu.VMEM((brows, rank), F32),
                pltpu.VMEM((SWEEPS + 1, 4, 2, brows, rank), BF16),
                pltpu.VMEM((SWEEPS, 4, 4, arows, rank), BF16),
                pltpu.VMEM((rank, ii), BF16),
                pltpu.VMEM((SWEEPS, 4, arows, rank), F32),
                pltpu.VMEM((4, arows, rank), F32),
                pltpu.VMEM((SWEEPS, 3, arows, rank), F32),
                pltpu.VMEM((2, rank, 2 * brows), F32),
                pltpu.VMEM((SWEEPS, 2, rank, 2 * brows), F32),
                pltpu.VMEM((2, 2, rank, brows), F32),
                pltpu.VMEM((SWEEPS, 3, rank, brows), F32),
                pltpu.VMEM((rank, rank), F32),
                pltpu.VMEM((SWEEPS + 1, rank, rank), F32),
                pltpu.VMEM((SWEEPS, 16, kk, rank), F32),
                pltpu.VMEM((kk, rank, rank), F32),
                pltpu.VMEM((rank, 2 * rank), F32),
                pltpu.VMEM((rank // 8, 8, 8, rank), F32),
                pltpu.VMEM((rank, 2 * rank), F32),
                pltpu.VMEM((rank, rank), F32),
                pltpu.VMEM((rank, rank), F32),
                pltpu.VMEM((rank, rank), F32),
                pltpu.VMEM(c_full.shape, F32),
                dma((kk,)), dma((3,)),
                *sems(SWEEPS, 3), *sems(SWEEPS, 9), *sems(SWEEPS, 3), *sems(SWEEPS, 2), *sems(SWEEPS, 3),
                *sems(SWEEPS + 1, 7), *sems(SWEEPS + 1, 2), *sems(SWEEPS, 15),
            ],
            compiler_params=pltpu.CompilerParams(
                collective_id=0, has_side_effects=True, vmem_limit_bytes=56 * 1024 * 1024
            ),
        )(x_blk, b_own, c_full, ridge_lam.reshape(1, 1))
        return split((arows, brows, crows), packed)

    return jax.shard_map(
        local_sweeps,
        mesh=mesh,
        in_specs=(P("tube", "row", "col"), P(("col", "row", "tube"), None), P(None, None), P()),
        out_specs=(P(("row", "col", "tube"), None), P(("col", "row", "tube"), None), P(None, None)),
        check_vma=False,
    )
```

```python
import jax
import jax.numpy as jnp
from jax import lax
from jax.experimental import pallas as pl
from jax.experimental.pallas import tpu as pltpu
from jax.sharding import PartitionSpec as P

SWEEPS = 2
HI = lax.Precision.HIGHEST
MESH = pl.DeviceIdType.MESH
F32 = jnp.float32
BF16 = jnp.bfloat16

YZ = [(1, 1, 0, 0), (0, 1, 0, 0), (1, 0, 0, 0)]
SAME_CORE = [(1, 0, 1, 0), (0, 0, 1, 0), (1, 0, 0, 0)]
YZ_FAR = [(1, 1, 1, 0), (0, 1, 1, 0), (1, 0, 1, 0), (0, 0, 1, 0)]
PARTNER = (0, 0, 0, 1)
ALL = YZ + [(t, c, x, k) for x, k in ((1, 1), (1, 0), (0, 1)) for c in (1, 0) for t in (1, 0)]


def dot_t0(a, b, **kw):
    return lax.dot_general(a, b, (((0,), (0,)), ((), ())), preferred_element_type=F32, **kw)


def kernel(
    x_hbm, b_hbm, c_hbm, lam_hbm,
    out,
    lam_ref, xf, xh, u_ref, b_in, bcols, a16, at_ref, af, pa, rsa, vp, vpr, vo, rsb, gbp, gbr, pc, cb,
    w_ref, e_ref, li_ref, inv_ref, ga_ref, gb_ref, cfac,
    x_sem, in_sem, rsa_s, rsa_r, aga_s, aga_r, af_s, af_r, vp_s, vp_r, rsb_s, rsb_r, agb_s, agb_r, gb_s, gb_r, pc_s, pc_r,
):
    t = lax.axis_index("tube")
    c = lax.axis_index("col")
    w = lax.axis_index("row")
    xc, core = w // 2, w % 2
    kk, ii, jj = xf.shape
    rank = b_in.shape[1]
    g = c * 2 + t
    me = g * 4 + w

    ins = [
        pltpu.make_async_copy(b_hbm, b_in, in_sem.at[0]),
        pltpu.make_async_copy(c_hbm, cfac, in_sem.at[1]),
        pltpu.make_async_copy(lam_hbm, lam_ref, in_sem.at[2]),
    ]
    for cp in ins:
        cp.start()
    depth = 5
    for k in range(depth):
        pltpu.make_async_copy(x_hbm.at[k], xf.at[k], x_sem.at[k]).start()

    def load(k, _):
        pltpu.make_async_copy(x_hbm.at[k], xf.at[k], x_sem.at[k]).wait()

        @pl.when(k + depth < kk)
        def _():
            pltpu.make_async_copy(x_hbm.at[k + depth], xf.at[k + depth], x_sem.at[k + depth]).start()

        for n in range(jj // ii):
            xh[k, n] = xf[k, :, n * ii : (n + 1) * ii].astype(BF16)
        return 0

    def dev(off):
        return ((t + off[0]) % 2, (c + off[1]) % 2, ((xc + off[2]) % 2) * 2 + (core + off[3]) % 2)

    barrier = pltpu.get_barrier_semaphore()
    for off in reversed(ALL):
        pl.semaphore_signal(barrier, inc=1, device_id=dev(off), device_id_type=MESH)
    ins[0].wait()
    bcols[0, w, t] = b_in[...].astype(BF16)
    first = 4
    lax.fori_loop(0, first, load, 0)
    pl.semaphore_wait(barrier, len(ALL))

    def push(src, dst, ss, rs, off):
        return pltpu.make_async_remote_copy(
            src_ref=src, dst_ref=dst, send_sem=ss, recv_sem=rs, device_id=dev(off), device_id_type=MESH
        )

    def b_copy(s, n, src, off):
        block = bcols.at[s, src[2], src[0]]
        return push(block, block, agb_s.at[s, n], agb_r.at[s, n], off)

    def gather_b(s):
        cps = [b_copy(s, n, (t, c, w), off) for n, off in enumerate(SAME_CORE + [PARTNER])]
        for cp in cps:
            cp.start()
        return cps

    def gram_part(s, k):
        bmat = jnp.concatenate([bcols[s, 2 * n + k].reshape(2 * rank, rank) for n in range(2)], axis=0)
        return dot_t0(bmat, bmat)

    def relay_b(s, cps):
        fwd = []
        for n, off in reversed(list(enumerate(SAME_CORE))):
            cps[n].wait()
            fwd.append(b_copy(s, 4 + n, dev(off), PARTNER))
            fwd[-1].start()
        cps[3].wait()
        gbp[...] = gram_part(s, core)
        for cp in fwd:
            cp.wait()
        gbp[...] += gram_part(s, 1 - core)
        for h in range(2):
            gram_copy(s, h).start()

    mid = rank // 2

    def gram_copy(s, h):
        part = pl.ds(h * mid, mid)
        return push(gbp.at[part], gbr.at[s, part], gb_s.at[s, h], gb_r.at[s, h], (0, 1, 0, 0))

    def gather_and_u(s, cps, each=lambda k, u: None):
        relay_b(s, cps)

        def body(k, _):
            acc = None
            for n in range(4):
                p = jnp.dot(xh[k, n], bcols[s, n].reshape(2 * rank, rank), preferred_element_type=F32)
                acc = p if acc is None else acc + p
            u_ref[k] = acc
            each(k, acc)
            return 0

        lax.fori_loop(0, kk, body, 0, unroll=8)

    def finish_gram_b(s, h):
        part = pl.ds(h * mid, mid)
        gram_copy(s, h).wait()
        gb_ref[part, :] = gbp[part, :] + gbr[s, part, :]

    def factor(gram_one, gram_two, ready=lambda h: None, by=4):
        rows = lax.broadcasted_iota(jnp.int32, (rank, rank), 0)
        cols = lax.broadcasted_iota(jnp.int32, (rank, rank), 1)
        eye = jnp.where(rows == cols, 1.0, 0.0).astype(F32)

        def fill(h):
            ready(h)
            part = slice(h * mid, (h + 1) * mid)
            w_ref[part, :rank] = gram_one[part, :] * gram_two[part, :] + lam_ref[0, 0] * eye[part, :]
            w_ref[part, rank:] = eye[part, :]

        r1 = lax.broadcasted_iota(jnp.int32, (8, rank), 0)

        def lane(x, n):
            return jnp.take_along_axis(x, jnp.full((8, rank), n, jnp.int32), axis=1, mode="promise_in_bounds")

        def spread(x, n):
            return jnp.broadcast_to(x[n : n + 1], (8, rank))

        def step(b, first, last):
            lo = pl.multiple_of(b * 8, 8)
            ps = w_ref[pl.ds(lo, 8), :rank]
            pi = w_ref[pl.ds(lo, 8), rank:]
            e = [lane(ps, lo + n) for n in range(8)]
            for n in range(8):
                for v in range(first, last):
                    e_ref[v, n] = lane(w_ref[8 * v : 8 * v + 8, :rank], lo + n)
            low_s = low_i = None
            piv = spread(e[0], 0)
            for j in range(8):
                isq = lax.rsqrt(piv)
                rc = isq * isq
                if j < 7:
                    x = spread(e[j + 1], j)
                    piv = spread(e[j + 1], j + 1) - (x * x) * rc
                m = e[j] * rc
                hit = r1 == j
                pjs = spread(ps, j)
                pji = spread(pi, j)
                low_s = pjs * isq if low_s is None else jnp.where(hit, pjs * isq, low_s)
                low_i = pji * isq if low_i is None else jnp.where(hit, pji * isq, low_i)
                ps = jnp.where(hit, pjs * rc, ps - m * pjs)
                pi = jnp.where(hit, pji * rc, pi - m * pji)
                for n in range(j + 1, 8):
                    en = spread(e[n], j)
                    e[n] = jnp.where(hit, en * rc, e[n] - m * en)
            li_ref[pl.ds(lo, 8), :rank] = low_s
            li_ref[pl.ds(lo, 8), rank:] = low_i
            qs = [spread(ps, n) for n in range(8)]
            qi = [spread(pi, n) for n in range(8)]
            for v in range(first, last):
                ds = [e_ref[v, n] * qs[n] for n in range(8)]
                di = [e_ref[v, n] * qi[n] for n in range(8)]
                while len(ds) > 1:
                    ds = [ds[n] + ds[n + 1] for n in range(0, len(ds), 2)]
                    di = [di[n] + di[n + 1] for n in range(0, len(di), 2)]
                w_ref[8 * v : 8 * v + 8, :rank] -= ds[0]
                w_ref[8 * v : 8 * v + 8, rank:] -= di[0]

        def run(lo, hi, first, last):
            def body(b, _):
                step(b, first, last)
                return 0

            lax.fori_loop(lo, hi, body, 0)

        half, end = rank // 16, rank // 8
        fill(0)
        for n in range(0, half, by):
            run(n, n + by, n, half)
        fill(1)
        w_ref[mid:, :] = w_ref[mid:, :] - dot_t0(li_ref[:mid, mid:rank], li_ref[:mid, :], precision=HI)
        for n in range(half, end, by):
            run(n, n + by, n, end)

    cps = gather_b(0)

    lax.fori_loop(first, kk, load, 0)
    for cp in ins[1:]:
        cp.wait()
    gather_and_u(0, cps)

    def sweep(s, _):
        c16 = cfac[...].astype(BF16)
        gram_c = dot_t0(c16, c16)

        def sum_rows(g2):
            part = pl.ds(pl.multiple_of(g2 * pa.shape[1], 8), pa.shape[1])

            def body(k, acc):
                return acc + u_ref[k, part, :] * cfac[pl.ds(t * kk + k, 1), :]

            pa[g2] = lax.fori_loop(0, kk, body, jnp.zeros(pa.shape[1:], F32), unroll=8)

        ra = []
        for n, off in enumerate(YZ):
            g2 = dev(off)[1] * 2 + dev(off)[0]
            sum_rows(g2)
            ra.append(push(pa.at[g2], rsa.at[s, n], rsa_s.at[s, n], rsa_r.at[s, n], off))
            ra[n].start()
        sum_rows(g)

        def ready_first(h):
            @pl.when(s == 0)
            def _():
                finish_gram_b(0, h)

        factor(gb_ref, gram_c, ready_first, by=2)
        inv_ref[...] = dot_t0(li_ref[:, rank:], li_ref[:, rank:], precision=HI)
        for cp in ra:
            cp.wait()
        mtt_a = pa[g] + rsa[s, 0] + rsa[s, 1] + rsa[s, 2]
        a_own = jnp.dot(mtt_a, inv_ref[...], precision=HI, preferred_element_type=F32)
        a16[s, w, g] = a_own.astype(BF16)
        af[s, g] = a_own
        ga = [
            push(a16.at[s, w, g], a16.at[s, w, g], aga_s.at[s, n], aga_r.at[s, n], off) for n, off in enumerate(YZ + YZ_FAR)
        ]
        for cp in ga:
            cp.start()
        out[: a_own.shape[0], :] = a_own

        cmine = cfac[pl.ds(pl.multiple_of(t * kk, kk), kk), :]
        ct = jnp.transpose(jnp.concatenate([cmine, jnp.zeros((rank - kk, rank), F32)], axis=0))
        for k in range(kk):
            cb[k] = jnp.broadcast_to(ct[:, k : k + 1], (rank, rank))
        for cp in ga[:3]:
            cp.wait()

        def hand_on(w2, n):
            return push(a16.at[s, w2], a16.at[s, w2], aga_s.at[s, n], aga_r.at[s, n], PARTNER)

        near = hand_on(w, 7)
        near.start()
        at_ref[...] = jnp.transpose(a16[s, w].reshape(ii, rank))

        def chunk(wc):
            def body(k, acc):
                ck = cb[k]
                return acc + jnp.dot(at_ref[...], xh[k, wc], preferred_element_type=F32) * jnp.concatenate([ck, ck], axis=1)

            return lax.fori_loop(0, kk, body, jnp.zeros((rank, ii), F32), unroll=16)

        vc = []
        for n in range(2):
            vp[n] = chunk(((xc + 1 - n) % 2) * 2 + (1 - core))
            vc.append(push(vp.at[n], vpr.at[s, n], vp_s.at[s, n], vp_r.at[s, n], (0, 0, 0, 1)))
            vc[n].start()
        for cp in ga[3:]:
            cp.wait()
        far = hand_on((1 - xc) * 2 + core, 8)
        far.start()
        rb = []
        for n in range(2):
            mine = chunk(((xc + 1 - n) % 2) * 2 + core)
            vc[n].wait()
            mine = mine + vpr[s, n]
            vo[n, 0] = mine[:, :rank]
            vo[n, 1] = mine[:, rank:]
            for off in ((1, 0, 1, 0), (0, 0, 1, 0)) if n == 0 else ((1, 0, 0, 0),):
                m = len(rb)
                rb.append(push(vo.at[n, dev(off)[0]], rsb.at[s, m], rsb_s.at[s, m], rsb_r.at[s, m], off))
                rb[m].start()
        fa = [push(af.at[s, g], af.at[s, g], af_s.at[s, n], af_r.at[s, n], off) for n, off in enumerate(YZ)]
        for cp in fa:
            cp.start()
        near.wait()
        far.wait()
        aall = a16[s].reshape(4 * ii, rank)
        ga_ref[...] = dot_t0(aall, aall)
        factor(ga_ref, gram_c)
        inv_ref[...] = dot_t0(li_ref[:, rank:], li_ref[:, rank:], precision=HI)
        for cp in rb:
            cp.wait()
        mtt_b = vo[1, t] + rsb[s, 0] + rsb[s, 1] + rsb[s, 2]
        b_own = jnp.transpose(jnp.dot(inv_ref[...], mtt_b, precision=HI, preferred_element_type=F32))
        bcols[s + 1, w, t] = b_own.astype(BF16)
        gcs = gather_b(s + 1)
        out[ii // 4 : ii // 4 + rank, :] = b_own

        for cp in fa:
            cp.wait()

        def part_c(k, u):
            pc[s, me, pl.ds(k, 1), :] = jnp.sum(u * af[s].reshape(ii, rank), axis=0, keepdims=True)

        gather_and_u(s + 1, gcs, part_c)
        cs = [push(pc.at[s, me], pc.at[s, me], pc_s.at[s, n], pc_r.at[s, n], off) for n, off in enumerate(ALL)]
        for cp in cs:
            cp.start()
        factor(ga_ref, gb_ref, lambda h: finish_gram_b(s + 1, h), by=2)
        inv_ref[...] = dot_t0(li_ref[:, rank:], li_ref[:, rank:], precision=HI)
        for cp in cs:
            cp.wait()
        halves = []
        for t2 in range(2):
            tot = None
            for c2 in range(2):
                for w2 in range(4):
                    term = pc[s, (c2 * 2 + t2) * 4 + w2]
                    tot = term if tot is None else tot + term
            halves.append(tot)
        cfac[...] = jnp.dot(jnp.concatenate(halves, axis=0), inv_ref[...], precision=HI, preferred_element_type=F32)
        return 0

    lax.fori_loop(0, SWEEPS, sweep, 0)
    out[ii // 4 + rank :, :] = cfac[...]


def split(rows, packed):
    def copy(src, *dsts):
        at = 0
        for n, dst in zip(rows, dsts):
            dst[...] = src[at : at + n, :]
            at += n

    vmem = pl.BlockSpec(memory_space=pltpu.VMEM)
    return pl.pallas_call(
        copy,
        name="results",
        out_shape=tuple(jax.ShapeDtypeStruct((n, packed.shape[1]), packed.dtype) for n in rows),
        in_specs=[vmem],
        out_specs=(vmem,) * len(rows),
        compiler_params=pltpu.CompilerParams(vmem_limit_bytes=1024 * 1024),
    )(packed)


def solution(mesh):
    def local_sweeps(x_blk, b_own, c_full, ridge_lam):
        kk, ii, jj = x_blk.shape
        brows, rank = b_own.shape
        arows, crows = ii // 4, c_full.shape[0]
        dma = pltpu.SemaphoreType.DMA
        vmem = pl.BlockSpec(memory_space=pltpu.VMEM)
        hbm = pl.BlockSpec(memory_space=pl.ANY)

        def sems(*shape):
            return [dma(shape), dma(shape)]

        packed = pl.pallas_call(
            kernel,
            name="als",
            out_shape=pltpu.VMEM((arows + brows + crows, rank), F32),
            in_specs=[hbm] * 4,
            out_specs=vmem,
            scratch_shapes=[
                pltpu.SMEM((1, 1), F32),
                pltpu.VMEM((kk, ii, jj), F32),
                pltpu.VMEM((kk, jj // ii, ii, ii), BF16),
                pltpu.VMEM((kk, ii, rank), F32),
                pltpu.VMEM((brows, rank), F32),
                pltpu.VMEM((SWEEPS + 1, 4, 2, brows, rank), BF16),
                pltpu.VMEM((SWEEPS, 4, 4, arows, rank), BF16),
                pltpu.VMEM((rank, ii), BF16),
                pltpu.VMEM((SWEEPS, 4, arows, rank), F32),
                pltpu.VMEM((4, arows, rank), F32),
                pltpu.VMEM((SWEEPS, 3, arows, rank), F32),
                pltpu.VMEM((2, rank, 2 * brows), F32),
                pltpu.VMEM((SWEEPS, 2, rank, 2 * brows), F32),
                pltpu.VMEM((2, 2, rank, brows), F32),
                pltpu.VMEM((SWEEPS, 3, rank, brows), F32),
                pltpu.VMEM((rank, rank), F32),
                pltpu.VMEM((SWEEPS + 1, rank, rank), F32),
                pltpu.VMEM((SWEEPS, 16, kk, rank), F32),
                pltpu.VMEM((kk, rank, rank), F32),
                pltpu.VMEM((rank, 2 * rank), F32),
                pltpu.VMEM((rank // 8, 8, 8, rank), F32),
                pltpu.VMEM((rank, 2 * rank), F32),
                pltpu.VMEM((rank, rank), F32),
                pltpu.VMEM((rank, rank), F32),
                pltpu.VMEM((rank, rank), F32),
                pltpu.VMEM(c_full.shape, F32),
                dma((kk,)), dma((3,)),
                *sems(SWEEPS, 3), *sems(SWEEPS, 9), *sems(SWEEPS, 3), *sems(SWEEPS, 2), *sems(SWEEPS, 3),
                *sems(SWEEPS + 1, 7), *sems(SWEEPS + 1, 2), *sems(SWEEPS, 15),
            ],
            compiler_params=pltpu.CompilerParams(
                collective_id=0, has_side_effects=True, vmem_limit_bytes=56 * 1024 * 1024
            ),
        )(x_blk, b_own, c_full, ridge_lam.reshape(1, 1))
        return split((arows, brows, crows), packed)

    return jax.shard_map(
        local_sweeps,
        mesh=mesh,
        in_specs=(P("tube", "row", "col"), P(("col", "row", "tube"), None), P(None, None), P()),
        out_specs=(P(("row", "col", "tube"), None), P(("col", "row", "tube"), None), P(None, None)),
        check_vma=False,
    )
```
